32 devices in a mesh: row: 4 (over y, core), phi: 8 (over z, x).
Axes of the slice: x: 2, y: 2, z: 4, core: 2. Of those that a mesh axis runs over, the one named last changes fastest.
Arguments:
- hydro_vars: float32 [5, 128, 128, 256], P(None, 'row', 'phi'), may hold values from -6 to 6
- face_b: float32 [3, 128, 128, 256], P(None, 'row', 'phi'), may hold values from -6 to 6
- widths: int32 [16], replicated, may hold values from 2 to 128, as said below
- diffusion: float32 [5, 256], replicated, may hold values from 0.01 to 0.06
Outputs:
- conserved: float32 [8, 128, 128, 256], P(None, 'row', 'phi')
- faces_out: float32 [3, 128, 128, 256], P(None, 'row', 'phi')
The draws below stay inside these ranges and needn't reach their ends.
Inputs may be any that keep to these rules, and one draw needn't show every extreme that they name: `widths`: every width is a power of two that divides 128; the two cycles next to the poles (entries 0 and 15) use 128.
All inputs are finite; a program needn't handle non-finite values.
Results may differ from the reference program's by a relative error of at most 0.0001.
Values sent between devices are 32-bit elements; how exact they have to be, the bound alone decides.
A program may use at most 64 MiB of HBM per device.

```python
import math
import jax
import jax.numpy as jnp
from jax import lax

NTH = 256
CYCLES = 8
NR = 128
PHI_CELLS = 128


def draw_widths(key, part):
    top = PHI_CELLS.bit_length() - 1
    powers = jax.random.randint(jax.random.fold_in(key, 7), (2 * CYCLES,), 1, top + 1)
    powers = powers.at[0].set(top).at[2 * CYCLES - 1].set(top)
    return jnp.power(2, powers).astype(jnp.int32)


def block_scale(rng, extent, pieces, low, high):
    loudness, own = 1.0, jax.random.fold_in(rng, 6)
    for position, blocks in pieces:
        draws = jnp.exp(jax.random.uniform(jax.random.fold_in(own, position), (blocks,), jnp.float32, low / len(pieces), high / len(pieces)))
        loudness = loudness * jnp.repeat(draws, extent[position] // blocks).reshape([-1 if axis == position else 1 for axis in range(len(extent))])
    return loudness


def centred(rng, extent, scale, limit, cuts=(), kind=jnp.bfloat16):
    values = jax.random.normal(rng, extent, jnp.float32) * scale
    if len(cuts) > 0:
        values = block_scale(rng, extent, cuts, -0.22, 0.18) * values
    return jnp.clip(values, min=-limit, max=limit).astype(kind)


def setup_inputs(seed: int = 0) -> dict:
    key_of = jax.random.split(jax.random.key(seed), 5)
    hydro_vars = centred(key_of[0], (5, NR, PHI_CELLS, NTH), 1.0, 6.0, ((1, 4), (2, 8)), jnp.float32)
    face_b = centred(key_of[1], (3, NR, PHI_CELLS, NTH), 1.0, 6.0, ((1, 4), (2, 8)), jnp.float32)
    widths = draw_widths(jax.random.fold_in(key_of[4], 71), 0)
    diffusion = jnp.clip(jnp.exp(jax.random.uniform(key_of[3], (5, NTH), jnp.float32, math.log(0.01), math.log(0.06))), 0.01, 0.06)
    return dict(hydro_vars=hydro_vars, face_b=face_b, widths=widths, diffusion=diffusion)


def stencil(padded, axis, count):
    parts = [lax.slice_in_dim(padded, offset, offset + count, axis=axis) for offset in range(5)]
    return (16.0 * (parts[1] + parts[3]) - (parts[0] + parts[4]) - 30.0 * parts[2]) / 12.0


def fourth(values, axis, wrapped):
    count = values.shape[axis]
    pads = [(0, 0)] * values.ndim
    pads[axis] = (2, 2)
    padded = jnp.pad(values, pads, mode="wrap") if wrapped else jnp.pad(values, pads)
    return stencil(padded, axis, count)


def block_means(cycles, axis, width):
    cells = cycles.shape[axis]
    result = cycles
    for power in range(1, cells.bit_length()):
        size = 2 ** power
        shape = cycles.shape[:axis] + (cells // size, size) + cycles.shape[axis + 1:]
        means = jnp.mean(cycles.reshape(shape), axis=axis + 1, keepdims=True)
        means = jnp.broadcast_to(means, shape).reshape(cycles.shape)
        result = jnp.where(width == size, means, result)
    return result


def reference(hydro_vars, face_b, widths, diffusion):
    fields = jnp.concatenate([hydro_vars, face_b], 0)
    theta_cells = fields.shape[3]
    polar_cycles = jnp.concatenate([fields[..., :CYCLES], fields[..., theta_cells - CYCLES:]], 3)
    averaged = block_means(polar_cycles, 2, widths)
    fields = jnp.concatenate([averaged[..., :CYCLES], fields[..., CYCLES:theta_cells - CYCLES], averaged[..., CYCLES:]], 3)
    hydro = fields[:5]
    change = fourth(hydro, 1, False) + fourth(hydro, 2, True) + fourth(hydro, 3, False)
    smoothed = hydro + diffusion[:, None, None, :] * change
    radial = fields[5]
    polar_face = fields[6]
    azimuth = fields[7]
    radial_next = jnp.concatenate([radial[1:], jnp.zeros_like(radial[:1])], 0)
    polar_next = jnp.concatenate([polar_face[..., 1:], jnp.zeros_like(polar_face[..., :1])], 2)
    azimuth_next = jnp.roll(azimuth, -1, axis=1)
    cell_field = 0.5 * jnp.stack([radial + radial_next, polar_face + polar_next, azimuth + azimuth_next])
    return jnp.concatenate([smoothed, cell_field], 0), fields[5:]
```

```python
import functools

import jax
import jax.numpy as jnp
from jax import lax
from jax.experimental import pallas as pl
from jax.experimental.pallas import tpu as pltpu
from jax.sharding import PartitionSpec as P

MESH = pl.DeviceIdType.MESH
LANES = 128
SUB = 8
EARLY = 2
LIMIT = 58000000


def kernel(
    nrow, nphi, rows, cells, tiles, cycles,
    widths_far, hydro, face, diffusion_far, O, F,
    H, S, R, SF, RF, FN, Q, M, PX, OM, MG, ELO, EHI, EL, ER,
    widths, diffusion, small_sem, load_sem, send_phi, recv_phi, send_edge, recv_edge,
    send_mean, recv_mean, send_row, recv_row, pair_ack, wrap_ack,
):
    nvar = hydro.shape[0]
    nface = face.shape[0]
    fields = nvar + nface
    last = tiles - 1
    blocks = cells // SUB
    ring = cells * tiles
    row = lax.axis_index("row")
    phi = lax.axis_index("phi")
    left = lax.rem(phi + nphi - 1, nphi)
    right = lax.rem(phi + 1, nphi)
    pairs = nphi // 2
    pair = phi // 2
    odd = lax.rem(phi, 2)
    partner = phi + 1 - 2 * odd
    far = jnp.where(odd == 1, right, left)
    near_way, far_way = 1 - odd, odd
    packed = 2 * cycles

    loads = [pltpu.make_async_copy(hydro.at[k], H.at[k, pl.ds(2 * ring, rows * ring)], load_sem.at[k]) for k in range(nvar)]
    loads += [pltpu.make_async_copy(face.at[k], F.at[k], load_sem.at[nvar + k]) for k in range(nface)]
    small = [
        pltpu.make_async_copy(widths_far, widths, small_sem.at[0]),
        pltpu.make_async_copy(diffusion_far, diffusion, small_sem.at[1]),
    ]
    for c in small + loads:
        c.start()

    barrier = pltpu.get_barrier_semaphore()

    def greet(**device):
        pl.semaphore_signal(barrier, inc=1, device_id=device, device_id_type=MESH)

    greet(phi=partner)

    @pl.when(phi < nphi - 1)
    def _():
        greet(phi=far)

    @pl.when(row > 0)
    def _():
        greet(row=row - 1)

    @pl.when(row < nrow - 1)
    def _():
        greet(row=row + 1)

    for step in range(1, pairs):

        @pl.when(pair + step < pairs)
        def _(step=step):
            greet(phi=phi + 2 * step)

    lane = lax.broadcasted_iota(jnp.int32, (1, LANES), 1)
    low = lane < cycles
    high = lane >= LANES - cycles
    mine = [(lane >= packed * f) & (lane < packed * (f + 1)) for f in range(fields)]

    def part(t):
        return slice(t * LANES, (t + 1) * LANES)

    def pack(value, f):
        return pltpu.roll(value, (cycles + packed * f) % LANES, 1)

    def unpack(value, f):
        return pltpu.roll(value, (-(cycles + packed * f)) % LANES, 1)

    def spot(r, b, t):
        start = r * ring + (b * tiles + t) * SUB
        return pl.ds(start if isinstance(r, int) else pl.multiple_of(start, SUB), SUB)

    def layer(r, cell, t):
        return pl.ds(r * ring + (cell // SUB * tiles + t) * SUB + cell % SUB, rows, stride=ring)

    def place(f):
        return (H, f, 2) if f < nvar else (F, f - nvar, 0)

    def halo(way, target, k):
        return pltpu.make_async_remote_copy(
            src_ref=S.at[way, k], dst_ref=R.at[way, k], send_sem=send_phi.at[way, k], recv_sem=recv_phi.at[way, k],
            device_id={"phi": target}, device_id_type=MESH)

    def near_copy(k):
        return halo(near_way, partner, k)

    def far_copy(k):
        return halo(far_way, far, k)

    mean_near = pltpu.make_async_remote_copy(
        src_ref=M, dst_ref=PX, send_sem=send_mean.at[0], recv_sem=recv_mean.at[0],
        device_id={"phi": partner}, device_id_type=MESH)

    def mean_copy(step):
        return pltpu.make_async_remote_copy(
            src_ref=MG.at[pair], dst_ref=MG.at[pair], send_sem=send_mean.at[step], recv_sem=recv_mean.at[step],
            device_id={"phi": lax.rem(phi + 2 * step, nphi)}, device_id_type=MESH)

    def pack_halo(k):
        for t in range(tiles):
            for i in range(2):
                S[0, k, i, t] = H[k, layer(2, i, t), :]
                S[1, k, i, t] = H[k, layer(2, cells - 2 + i, t), :]

    for k in range(nvar):
        loads[k].wait()
        pack_halo(k)
        if k == 0:
            known = 1 + jnp.where(phi > 0, 1, 0) + pair
            known = known + jnp.where(row > 0, 1, 0) + jnp.where(row < nrow - 1, 1, 0)
            pl.semaphore_wait(barrier, known)
            for step in range(1, pairs):

                @pl.when(pair >= step)
                def _(step=step):
                    pl.semaphore_signal(pair_ack.at[step], inc=1, device_id={"phi": phi - 2 * step}, device_id_type=MESH)

            @pl.when(phi == nphi - 1)
            def _():
                pl.semaphore_signal(wrap_ack, inc=1, device_id={"phi": 0}, device_id_type=MESH)

        if k < EARLY:
            near_copy(k).start()
    for c in loads[nvar:]:
        c.wait()

    def polar_cells(r, b):
        value = jnp.zeros((SUB, LANES), jnp.float32)
        for f in range(fields):
            ref, k, base = place(f)
            polar = jnp.where(low, ref[k, spot(r + base, b, 0), :], ref[k, spot(r + base, b, last), :])
            value = jnp.where(mine[f], pack(polar, f), value)
        return value

    def cell_mean(r, carry):
        value = jnp.zeros((SUB, LANES), jnp.float32)
        for f in range(fields):
            ref, k, base = place(f)
            sums = [ref[k, spot(r + base, 0, t), :] for t in (0, last)]
            for b in range(1, blocks):
                sums = [x + ref[k, spot(r + base, b, t), :] for x, t in zip(sums, (0, last))]
            value = jnp.where(mine[f], pack(jnp.where(low, sums[0], sums[1]), f), value)
        size = SUB // 2
        while size:
            value = value + pltpu.roll(value, size, 0)
            size //= 2
        M[pl.ds(r, 1), :] = value[0:1] * (1.0 / cells)
        return carry

    lax.fori_loop(0, rows, cell_mean, 0, unroll=4)
    mean_near.start()

    @pl.when(phi > 0)
    def _():
        for k in range(EARLY):
            far_copy(k).start()

    for k in range(EARLY, nvar):
        near_copy(k).start()
    for t in range(tiles):
        SF[t] = F[nface - 1, layer(0, 0, t), :]

    for c in small:
        c.wait()
    width = jnp.zeros((1, LANES), jnp.int32)
    slot = lax.rem(lane, packed)
    for j in range(cycles):
        width = jnp.where(slot == cycles + j, widths[j], width)
        width = jnp.where(slot == j, widths[cycles + j], width)

    index = lax.broadcasted_iota(jnp.int32, (SUB, LANES), 0)

    def local_average(r, carry):
        totals = [polar_cells(r, b) for b in range(blocks)]
        results = list(totals)
        size = 1
        while size < cells:
            if size < SUB:
                turned = []
                for v in totals:
                    forward = pltpu.roll(v, SUB - size, 0)
                    if 2 * size < SUB:
                        forward = jnp.where((index & size) == 0, forward, pltpu.roll(v, size, 0))
                    turned.append(v + forward)
                totals = turned
            else:
                hop = size // SUB
                totals = [totals[b] + totals[b ^ hop] for b in range(blocks)]
            size *= 2
            results = [jnp.where(width == size, v * (1.0 / size), old) for v, old in zip(totals, results)]
        for b in range(blocks):
            Q[pl.ds(pl.multiple_of(r * cells + b * SUB, SUB), SUB), :] = results[b]
        ELO[pl.ds(r, 1), :] = results[0][0:1]
        EHI[pl.ds(r, 1), :] = results[blocks - 1][SUB - 1 : SUB]
        return carry

    lax.fori_loop(0, rows, local_average, 0, unroll=2)

    edge_left = pltpu.make_async_remote_copy(
        src_ref=ELO, dst_ref=ER, send_sem=send_edge.at[0], recv_sem=recv_edge.at[0],
        device_id={"phi": left}, device_id_type=MESH)
    edge_right = pltpu.make_async_remote_copy(
        src_ref=EHI, dst_ref=EL, send_sem=send_edge.at[1], recv_sem=recv_edge.at[1],
        device_id={"phi": right}, device_id_type=MESH)
    face_left = pltpu.make_async_remote_copy(
        src_ref=SF, dst_ref=RF, send_sem=send_edge.at[2], recv_sem=recv_edge.at[2],
        device_id={"phi": left}, device_id_type=MESH)
    mean_near.wait_recv()
    MG[pair] = (M[...] + PX[...]) * 0.5
    for step in range(1, pairs):

        @pl.when(pair + step < pairs)
        def _(step=step):
            pl.semaphore_wait(pair_ack.at[step], 1)

        mean_copy(step).start()

    @pl.when(phi == 0)
    def _():
        pl.semaphore_wait(wrap_ack, 1)
        for k in range(EARLY):
            far_copy(k).start()

    for k in range(EARLY, nvar):
        far_copy(k).start()
    edge_left.start()
    edge_right.start()
    face_left.start()

    for step in range(1, pairs):
        mean_copy(step).wait_recv()

    def group_mean(who):
        result = MG[who // 2]
        size = 2
        while size <= pairs:
            start = (who // (2 * size)) * size
            total = MG[start]
            for i in range(1, size):
                total = total + MG[start + i]
            result = jnp.where(width == 2 * size * cells, total * (1.0 / size), result)
            size *= 2
        return result

    OM[...] = group_mean(phi)
    next_lo = group_mean(right)
    next_hi = group_mean(left)
    wide = width > cells

    def spread(r):
        mean = jnp.broadcast_to(OM[pl.ds(r, 1), :], (SUB, LANES))
        for b in range(blocks):
            where = pl.ds(r * cells + b * SUB if isinstance(r, int) else pl.multiple_of(r * cells + b * SUB, SUB), SUB)
            value = jnp.where(wide, mean, Q[where, :])
            for f in range(fields):
                ref, k, base = place(f)
                polar = unpack(value, f)
                ref[k, spot(r + base, b, 0), :] = jnp.where(low, polar, ref[k, spot(r + base, b, 0), :])
                ref[k, spot(r + base, b, last), :] = jnp.where(high, polar, ref[k, spot(r + base, b, last), :])

    for r in (0, 1, rows - 2, rows - 1):
        spread(r)
    lax.fori_loop(2, rows - 2, lambda r, c: (spread(r), c)[1], 0, unroll=4)

    down = pltpu.make_async_remote_copy(
        src_ref=H.at[:, pl.ds(2 * ring, 2 * ring)], dst_ref=H.at[:, pl.ds((rows + 2) * ring, 2 * ring)],
        send_sem=send_row.at[0], recv_sem=recv_row.at[0], device_id={"row": row - 1}, device_id_type=MESH)
    down_face = pltpu.make_async_remote_copy(
        src_ref=F.at[0, pl.ds(0, ring)], dst_ref=FN,
        send_sem=send_row.at[1], recv_sem=recv_row.at[1], device_id={"row": row - 1}, device_id_type=MESH)
    up = pltpu.make_async_remote_copy(
        src_ref=H.at[:, pl.ds(rows * ring, 2 * ring)], dst_ref=H.at[:, pl.ds(0, 2 * ring)],
        send_sem=send_row.at[2], recv_sem=recv_row.at[2], device_id={"row": row + 1}, device_id_type=MESH)

    @pl.when(row > 0)
    def _():
        down.start()
        down_face.start()

    @pl.when(row < nrow - 1)
    def _():
        up.start()

    @pl.when(row == 0)
    def _():
        H[:, pl.ds(0, 2 * ring), :] = jnp.zeros((nvar, 2 * ring, LANES), jnp.float32)

    @pl.when(row == nrow - 1)
    def _():
        H[:, pl.ds((rows + 2) * ring, 2 * ring), :] = jnp.zeros((nvar, 2 * ring, LANES), jnp.float32)
        FN[...] = jnp.zeros_like(FN)

    def whole(ref, k, r, t):
        return jnp.concatenate([ref[k, spot(r, b, t), :] for b in range(blocks)], 0)

    def write(k, r, t, value):
        for b in range(blocks):
            O[k, spot(r, b, t), :] = value[b * SUB : (b + 1) * SUB]

    def shifted(parts, amount):
        out = []
        turned = [pltpu.roll(p, (-amount) % LANES, 1) for p in parts]
        for t in range(tiles):
            if amount > 0:
                inside = lane < LANES - amount
                other = turned[t + 1] if t + 1 < tiles else 0.0
            else:
                inside = lane >= -amount
                other = turned[t - 1] if t > 0 else 0.0
            out.append(jnp.where(inside, turned[t], other))
        return out

    def smooth_row(r):
        for k in range(nvar):
            mid = [whole(H, k, r + 2, t) for t in range(tiles)]
            one = [a + b for a, b in zip(shifted(mid, 1), shifted(mid, -1))]
            two = [a + b for a, b in zip(shifted(mid, 2), shifted(mid, -2))]
            for t in range(tiles):
                v = mid[t]
                s1 = one[t] + (pltpu.roll(v, 1, 0) + pltpu.roll(v, cells - 1, 0)) + (whole(H, k, r + 1, t) + whole(H, k, r + 3, t))
                s2 = two[t] + (pltpu.roll(v, 2, 0) + pltpu.roll(v, cells - 2, 0)) + (whole(H, k, r, t) + whole(H, k, r + 4, t))
                change = (16.0 * s1 - s2 - 90.0 * v) * (1.0 / 12.0)
                write(k, r, t, v + diffusion[k : k + 1, part(t)] * change)

    def field_row(r, following):
        polar = [whole(F, 1, r, t) for t in range(tiles)]
        polar_next = shifted(polar, 1)
        for t in range(tiles):
            write(nvar, r, t, 0.5 * (whole(F, 0, r, t) + following(t)))
            write(nvar + 1, r, t, 0.5 * (polar[t] + polar_next[t]))
            azimuth = whole(F, 2, r, t)
            write(nvar + 2, r, t, 0.5 * (azimuth + pltpu.roll(azimuth, cells - 1, 0)))

    def inner_row(r, carry):
        field_row(r, lambda t: whole(F, 0, r + 1, t))
        smooth_row(r)
        return carry

    lax.fori_loop(2, rows - 2, inner_row, 0, unroll=2)
    for r in (0, 1, rows - 2):
        field_row(r, lambda t, r=r: whole(F, 0, r + 1, t))

    @pl.when(row > 0)
    def _():
        up.wait_recv()

    @pl.when(row < nrow - 1)
    def _():
        down.wait_recv()
        down_face.wait_recv()

    field_row(rows - 1, lambda t: jnp.concatenate([FN[spot(0, b, t), :] for b in range(blocks)], 0))
    for r in (0, 1, rows - 2, rows - 1):
        smooth_row(r)

    edge_left.wait_recv()
    edge_right.wait_recv()
    local = width <= cells
    from_left = jnp.where(local, EL[...], next_hi)
    from_right = jnp.where(local, ER[...], next_lo)

    def fixed(raw, edge, t):
        if t == 0:
            raw = jnp.where(low, edge, raw)
        if t == last:
            raw = jnp.where(high, edge, raw)
        return raw

    for k in range(nvar):
        halo(1, right, k).wait_recv()
        halo(0, left, k).wait_recv()
        edge_l = unpack(from_left, k)
        edge_r = unpack(from_right, k)
        for t in range(tiles):
            scale = diffusion[k : k + 1, part(t)] * (1.0 / 12.0)
            l1 = fixed(R[1, k, 1, t], edge_l, t) - H[k, layer(2, cells - 1, t), :]
            l2 = fixed(R[1, k, 0, t], edge_l, t) - H[k, layer(2, cells - 2, t), :]
            r1 = fixed(R[0, k, 0, t], edge_r, t) - H[k, layer(2, 0, t), :]
            r2 = fixed(R[0, k, 1, t], edge_r, t) - H[k, layer(2, 1, t), :]
            for cell, term in ((0, 16.0 * l1 - l2), (1, -l1), (cells - 2, -r1), (cells - 1, 16.0 * r1 - r2)):
                O[k, layer(0, cell, t), :] = O[k, layer(0, cell, t), :] + scale * term

    face_left.wait_recv()
    edge_f = unpack(from_right, fields - 1)
    for t in range(tiles):
        O[fields - 1, layer(0, cells - 1, t), :] = 0.5 * (F[nface - 1, layer(0, cells - 1, t), :] + fixed(RF[t], edge_f, t))

    for k in range(nvar):
        near_copy(k).wait_send()
        far_copy(k).wait_send()
    edge_left.wait_send()
    edge_right.wait_send()
    face_left.wait_send()
    mean_near.wait_send()
    for step in range(1, pairs):
        mean_copy(step).wait_send()

    @pl.when(row > 0)
    def _():
        down.wait_send()
        down_face.wait_send()

    @pl.when(row < nrow - 1)
    def _():
        up.wait_send()


def spill(pieces, conserved, faces, conserved_out, faces_out, sem):
    fields = conserved.shape[0]
    size = conserved.shape[1] // pieces
    copies = []
    for k in range(fields + faces.shape[0]):
        source, target, i = (conserved, conserved_out, k) if k < fields else (faces, faces_out, k - fields)
        for p in range(pieces):
            where = pl.ds(p * size, size)
            copies.append(pltpu.make_async_copy(source.at[i, where], target.at[i, where], sem.at[k, p]))
    for c in copies:
        c.start()
    for c in copies:
        c.wait()


def blocked(x):
    n, rows, cells, theta = x.shape
    x = x.reshape(n, rows, cells // SUB, SUB, theta // LANES, LANES)
    return x.transpose(0, 1, 2, 4, 3, 5).reshape(n, rows * cells * (theta // LANES), LANES)


def unblocked(x, rows, cells, theta):
    x = x.reshape(x.shape[0], rows, cells // SUB, theta // LANES, SUB, LANES)
    return x.transpose(0, 1, 2, 4, 3, 5).reshape(x.shape[0], rows, cells, theta)


def body(nrow, nphi, hydro_vars, face_b, widths, diffusion):
    nvar, rows, cells, theta = hydro_vars.shape
    nface = face_b.shape[0]
    fields = nvar + nface
    cycles = widths.shape[0] // 2
    tiles = theta // LANES
    ring = cells * tiles
    f32 = jnp.float32
    shape = lambda *s: pltpu.VMEM(s, f32)
    far = pl.BlockSpec(memory_space=pltpu.HBM)
    near = pl.BlockSpec(memory_space=pltpu.VMEM)
    result_bytes = (fields + nface) * rows * ring * LANES * 4
    conserved, faces = pl.pallas_call(
        functools.partial(kernel, nrow, nphi, rows, cells, tiles, cycles),
        out_shape=(
            pltpu.VMEM((fields, rows * ring, LANES), f32),
            pltpu.VMEM((nface, rows * ring, LANES), f32),
        ),
        in_specs=[far, far, far, far],
        out_specs=(near, near),
        scratch_shapes=[
            shape(nvar, (rows + 4) * ring, LANES),
            shape(2, nvar, 2, tiles, rows, LANES),
            shape(2, nvar, 2, tiles, rows, LANES),
            shape(tiles, rows, LANES),
            shape(tiles, rows, LANES),
            shape(ring, LANES),
            shape(rows * cells, LANES),
            shape(rows, LANES),
            shape(rows, LANES),
            shape(rows, LANES),
            shape(nphi // 2, rows, LANES),
            shape(rows, LANES),
            shape(rows, LANES),
            shape(rows, LANES),
            shape(rows, LANES),
            pltpu.SMEM((2 * cycles,), jnp.int32),
            shape(nvar, theta),
            pltpu.SemaphoreType.DMA((2,)),
            pltpu.SemaphoreType.DMA((fields,)),
            pltpu.SemaphoreType.DMA((2, nvar)),
            pltpu.SemaphoreType.DMA((2, nvar)),
            pltpu.SemaphoreType.DMA((3,)),
            pltpu.SemaphoreType.DMA((3,)),
            pltpu.SemaphoreType.DMA((nphi // 2,)),
            pltpu.SemaphoreType.DMA((nphi // 2,)),
            pltpu.SemaphoreType.DMA((3,)),
            pltpu.SemaphoreType.DMA((3,)),
            pltpu.SemaphoreType.REGULAR((nphi // 2,)),
            pltpu.SemaphoreType.REGULAR,
        ],
        compiler_params=pltpu.CompilerParams(
            collective_id=0, has_side_effects=True, vmem_limit_bytes=LIMIT - result_bytes
        ),
        name="step",
    )(widths, blocked(hydro_vars), blocked(face_b), diffusion)
    pieces = 2
    conserved, faces = pl.pallas_call(
        functools.partial(spill, pieces),
        out_shape=(
            jax.ShapeDtypeStruct((fields, rows * ring, LANES), f32),
            jax.ShapeDtypeStruct((nface, rows * ring, LANES), f32),
        ),
        in_specs=[near, near],
        out_specs=(far, far),
        scratch_shapes=[pltpu.SemaphoreType.DMA((fields + nface, pieces))],
        compiler_params=pltpu.CompilerParams(vmem_limit_bytes=1000000),
        name="spill",
    )(conserved, faces)
    return unblocked(conserved, rows, cells, theta), unblocked(faces, rows, cells, theta)


def solution(mesh):
    spec = P(None, "row", "phi", None)
    return jax.shard_map(
        functools.partial(body, mesh.shape["row"], mesh.shape["phi"]),
        mesh=mesh,
        in_specs=(spec, spec, P(), P()),
        out_specs=(spec, spec),
        check_vma=False,
    )
```

```python
import functools

import jax
import jax.numpy as jnp
from jax import lax
from jax.experimental import pallas as pl
from jax.experimental.pallas import tpu as pltpu
from jax.sharding import PartitionSpec as P

MESH = pl.DeviceIdType.MESH
LANES = 128
SUB = 8
EARLY = 1
MIDDLE = 2
LIMIT = 58000000


def kernel(
    nrow, nphi, rows, cells, tiles, cycles,
    widths_far, hydro, face, diffusion_far, O, F,
    H, S, R, SF, RF, FN, Q, M, PX, OM, MG, E, EX,
    widths, diffusion, small_sem, load_sem, send_phi, recv_phi, send_edge, recv_edge,
    send_mean, recv_mean, send_row, recv_row, pair_ack, far_ack, row_ack,
):
    nvar = hydro.shape[0]
    nface = face.shape[0]
    fields = nvar + nface
    last = tiles - 1
    blocks = cells // SUB
    ring = cells * tiles
    row = lax.axis_index("row")
    phi = lax.axis_index("phi")
    left = lax.rem(phi + nphi - 1, nphi)
    right = lax.rem(phi + 1, nphi)
    pairs = nphi // 2
    pair = phi // 2
    odd = lax.rem(phi, 2)
    partner = phi + 1 - 2 * odd
    far = jnp.where(odd == 1, right, left)
    near_way, far_way = 1 - odd, odd
    packed = 2 * cycles

    loads = [pltpu.make_async_copy(hydro.at[k], H.at[k, pl.ds(2 * ring, rows * ring)], load_sem.at[k]) for k in range(nvar)]
    loads += [pltpu.make_async_copy(face.at[k], F.at[k], load_sem.at[nvar + k]) for k in range(nface)]
    small = [
        pltpu.make_async_copy(widths_far, widths, small_sem.at[0]),
        pltpu.make_async_copy(diffusion_far, diffusion, small_sem.at[1]),
    ]
    for c in small + loads:
        c.start()

    barrier = pltpu.get_barrier_semaphore()

    def greet(**device):
        pl.semaphore_signal(barrier, inc=1, device_id=device, device_id_type=MESH)

    greet(phi=partner)

    @pl.when(far > phi)
    def _():
        greet(phi=far)

    @pl.when(row < nrow - 1)
    def _():
        greet(row=row + 1)

    for step in range(1, pairs):

        @pl.when(pair + step < pairs)
        def _(step=step):
            greet(phi=phi + 2 * step)

    lane = lax.broadcasted_iota(jnp.int32, (1, LANES), 1)
    low = lane < cycles
    high = lane >= LANES - cycles
    mine = [(lane >= packed * f) & (lane < packed * (f + 1)) for f in range(fields)]

    def part(t):
        return slice(t * LANES, (t + 1) * LANES)

    def pack(value, f):
        return pltpu.roll(value, (cycles + packed * f) % LANES, 1)

    def unpack(value, f):
        return pltpu.roll(value, (-(cycles + packed * f)) % LANES, 1)

    def spot(r, b, t):
        start = r * ring + (b * tiles + t) * SUB
        return pl.ds(start if isinstance(r, int) else pl.multiple_of(start, SUB), SUB)

    def layer(r, cell, t):
        return pl.ds(r * ring + (cell // SUB * tiles + t) * SUB + cell % SUB, rows, stride=ring)

    def place(f):
        return (H, f, 2) if f < nvar else (F, f - nvar, 0)

    def halo(way, target, k):
        return pltpu.make_async_remote_copy(
            src_ref=S.at[way, k], dst_ref=R.at[way, k], send_sem=send_phi.at[way, k], recv_sem=recv_phi.at[way, k],
            device_id={"phi": target}, device_id_type=MESH)

    def near_copy(k):
        return halo(near_way, partner, k)

    def far_copy(k):
        return halo(far_way, far, k)

    mean_near = pltpu.make_async_remote_copy(
        src_ref=M, dst_ref=PX, send_sem=send_mean.at[0], recv_sem=recv_mean.at[0],
        device_id={"phi": partner}, device_id_type=MESH)

    def mean_copy(step):
        return pltpu.make_async_remote_copy(
            src_ref=MG.at[pair], dst_ref=MG.at[pair], send_sem=send_mean.at[step], recv_sem=recv_mean.at[step],
            device_id={"phi": lax.rem(phi + 2 * step, nphi)}, device_id_type=MESH)

    def pack_halo(k):
        for t in range(tiles):
            for i in range(2):
                S[0, k, i, t] = H[k, layer(2, i, t), :]
                S[1, k, i, t] = H[k, layer(2, cells - 2 + i, t), :]

    for k in range(nvar):
        loads[k].wait()
        pack_halo(k)
        if k == 0:
            known = 1 + jnp.where(far < phi, 1, 0) + pair + jnp.where(row > 0, 1, 0)
            pl.semaphore_wait(barrier, known)
            for step in range(1, pairs):

                @pl.when(pair >= step)
                def _(step=step):
                    pl.semaphore_signal(pair_ack.at[step], inc=1, device_id={"phi": phi - 2 * step}, device_id_type=MESH)

            @pl.when(far < phi)
            def _():
                pl.semaphore_signal(far_ack, inc=1, device_id={"phi": far}, device_id_type=MESH)

            @pl.when(row > 0)
            def _():
                pl.semaphore_signal(row_ack, inc=1, device_id={"row": row - 1}, device_id_type=MESH)

        if k < EARLY:
            near_copy(k).start()
    for c in loads[nvar:]:
        c.wait()

    def polar_cells(r, b):
        value = jnp.zeros((SUB, LANES), jnp.float32)
        for f in range(fields):
            ref, k, base = place(f)
            polar = jnp.where(low, ref[k, spot(r + base, b, 0), :], ref[k, spot(r + base, b, last), :])
            value = jnp.where(mine[f], pack(polar, f), value)
        return value

    def cell_mean(r, carry):
        value = jnp.zeros((SUB, LANES), jnp.float32)
        for f in range(fields):
            ref, k, base = place(f)
            sums = [ref[k, spot(r + base, 0, t), :] for t in (0, last)]
            for b in range(1, blocks):
                sums = [x + ref[k, spot(r + base, b, t), :] for x, t in zip(sums, (0, last))]
            value = jnp.where(mine[f], pack(jnp.where(low, sums[0], sums[1]), f), value)
        size = SUB // 2
        while size:
            value = value + pltpu.roll(value, size, 0)
            size //= 2
        M[pl.ds(r, 1), :] = value[0:1] * (1.0 / cells)
        return carry

    lax.fori_loop(0, rows, cell_mean, 0, unroll=4)
    mean_near.start()
    for k in range(EARLY, MIDDLE):
        near_copy(k).start()
    for t in range(tiles):
        SF[t] = F[nface - 1, layer(0, 0, t), :]

    for c in small:
        c.wait()
    width = jnp.zeros((1, LANES), jnp.int32)
    slot = lax.rem(lane, packed)
    for j in range(cycles):
        width = jnp.where(slot == cycles + j, widths[j], width)
        width = jnp.where(slot == j, widths[cycles + j], width)

    index = lax.broadcasted_iota(jnp.int32, (SUB, LANES), 0)

    def local_average(r, carry):
        totals = [polar_cells(r, b) for b in range(blocks)]
        results = list(totals)
        size = 1
        while size < cells:
            if size < SUB:
                turned = []
                for v in totals:
                    forward = pltpu.roll(v, SUB - size, 0)
                    if 2 * size < SUB:
                        forward = jnp.where((index & size) == 0, forward, pltpu.roll(v, size, 0))
                    turned.append(v + forward)
                totals = turned
            else:
                hop = size // SUB
                totals = [totals[b] + totals[b ^ hop] for b in range(blocks)]
            size *= 2
            results = [jnp.where(width == size, v * (1.0 / size), old) for v, old in zip(totals, results)]
        for b in range(blocks):
            Q[pl.ds(pl.multiple_of(r * cells + b * SUB, SUB), SUB), :] = results[b]
        E[0, pl.ds(r, 1), :] = results[0][0:1]
        E[1, pl.ds(r, 1), :] = results[blocks - 1][SUB - 1 : SUB]
        return carry

    lax.fori_loop(0, rows, local_average, 0, unroll=2)

    def edge_copy(way, target):
        return pltpu.make_async_remote_copy(
            src_ref=E.at[way], dst_ref=EX.at[way], send_sem=send_edge.at[way], recv_sem=recv_edge.at[way],
            device_id={"phi": target}, device_id_type=MESH)

    face_left = pltpu.make_async_remote_copy(
        src_ref=SF, dst_ref=RF, send_sem=send_edge.at[2], recv_sem=recv_edge.at[2],
        device_id={"phi": left}, device_id_type=MESH)
    edge_copy(near_way, partner).start()

    @pl.when(odd == 1)
    def _():
        face_left.start()

    for k in range(MIDDLE, nvar):
        near_copy(k).start()

    mean_near.wait_recv()
    MG[pair] = (M[...] + PX[...]) * 0.5
    for step in range(1, pairs):

        @pl.when(pair + step < pairs)
        def _(step=step):
            pl.semaphore_wait(pair_ack.at[step], 1)

        mean_copy(step).start()

    @pl.when(far > phi)
    def _():
        pl.semaphore_wait(far_ack, 1)

    edge_copy(far_way, far).start()

    @pl.when(odd == 0)
    def _():
        face_left.start()

    for k in range(nvar):
        far_copy(k).start()

    for step in range(1, pairs):
        mean_copy(step).wait_recv()

    def group_mean(who):
        result = MG[who // 2]
        size = 2
        while size <= pairs:
            start = (who // (2 * size)) * size
            total = MG[start]
            for i in range(1, size):
                total = total + MG[start + i]
            result = jnp.where(width == 2 * size * cells, total * (1.0 / size), result)
            size *= 2
        return result

    OM[...] = group_mean(phi)
    next_lo = group_mean(right)
    next_hi = group_mean(left)
    wide = width > cells

    def spread(r):
        mean = jnp.broadcast_to(OM[pl.ds(r, 1), :], (SUB, LANES))
        for b in range(blocks):
            where = pl.ds(r * cells + b * SUB if isinstance(r, int) else pl.multiple_of(r * cells + b * SUB, SUB), SUB)
            value = jnp.where(wide, mean, Q[where, :])
            for f in range(fields):
                ref, k, base = place(f)
                polar = unpack(value, f)
                ref[k, spot(r + base, b, 0), :] = jnp.where(low, polar, ref[k, spot(r + base, b, 0), :])
                ref[k, spot(r + base, b, last), :] = jnp.where(high, polar, ref[k, spot(r + base, b, last), :])

    for r in (0, 1, rows - 2, rows - 1):
        spread(r)
    lax.fori_loop(2, rows - 2, lambda r, c: (spread(r), c)[1], 0, unroll=4)

    down = pltpu.make_async_remote_copy(
        src_ref=H.at[:, pl.ds(2 * ring, 2 * ring)], dst_ref=H.at[:, pl.ds((rows + 2) * ring, 2 * ring)],
        send_sem=send_row.at[0], recv_sem=recv_row.at[0], device_id={"row": row - 1}, device_id_type=MESH)
    down_face = pltpu.make_async_remote_copy(
        src_ref=F.at[0, pl.ds(0, ring)], dst_ref=FN,
        send_sem=send_row.at[1], recv_sem=recv_row.at[1], device_id={"row": row - 1}, device_id_type=MESH)
    up = pltpu.make_async_remote_copy(
        src_ref=H.at[:, pl.ds(rows * ring, 2 * ring)], dst_ref=H.at[:, pl.ds(0, 2 * ring)],
        send_sem=send_row.at[2], recv_sem=recv_row.at[2], device_id={"row": row + 1}, device_id_type=MESH)

    @pl.when(row > 0)
    def _():
        down.start()
        down_face.start()

    @pl.when(row < nrow - 1)
    def _():
        pl.semaphore_wait(row_ack, 1)
        up.start()

    @pl.when(row == 0)
    def _():
        H[:, pl.ds(0, 2 * ring), :] = jnp.zeros((nvar, 2 * ring, LANES), jnp.float32)

    @pl.when(row == nrow - 1)
    def _():
        H[:, pl.ds((rows + 2) * ring, 2 * ring), :] = jnp.zeros((nvar, 2 * ring, LANES), jnp.float32)
        FN[...] = jnp.zeros_like(FN)

    def whole(ref, k, r, t):
        return jnp.concatenate([ref[k, spot(r, b, t), :] for b in range(blocks)], 0)

    def write(k, r, t, value):
        for b in range(blocks):
            O[k, spot(r, b, t), :] = value[b * SUB : (b + 1) * SUB]

    def shifted(parts, amount):
        out = []
        turned = [pltpu.roll(p, (-amount) % LANES, 1) for p in parts]
        for t in range(tiles):
            if amount > 0:
                inside = lane < LANES - amount
                other = turned[t + 1] if t + 1 < tiles else 0.0
            else:
                inside = lane >= -amount
                other = turned[t - 1] if t > 0 else 0.0
            out.append(jnp.where(inside, turned[t], other))
        return out

    def smooth_row(r):
        for k in range(nvar):
            mid = [whole(H, k, r + 2, t) for t in range(tiles)]
            one = [a + b for a, b in zip(shifted(mid, 1), shifted(mid, -1))]
            two = [a + b for a, b in zip(shifted(mid, 2), shifted(mid, -2))]
            for t in range(tiles):
                v = mid[t]
                s1 = one[t] + (pltpu.roll(v, 1, 0) + pltpu.roll(v, cells - 1, 0)) + (whole(H, k, r + 1, t) + whole(H, k, r + 3, t))
                s2 = two[t] + (pltpu.roll(v, 2, 0) + pltpu.roll(v, cells - 2, 0)) + (whole(H, k, r, t) + whole(H, k, r + 4, t))
                change = (16.0 * s1 - s2 - 90.0 * v) * (1.0 / 12.0)
                write(k, r, t, v + diffusion[k : k + 1, part(t)] * change)

    def field_row(r, following):
        polar = [whole(F, 1, r, t) for t in range(tiles)]
        polar_next = shifted(polar, 1)
        for t in range(tiles):
            write(nvar, r, t, 0.5 * (whole(F, 0, r, t) + following(t)))
            write(nvar + 1, r, t, 0.5 * (polar[t] + polar_next[t]))
            azimuth = whole(F, 2, r, t)
            write(nvar + 2, r, t, 0.5 * (azimuth + pltpu.roll(azimuth, cells - 1, 0)))

    def inner_row(r, carry):
        field_row(r, lambda t: whole(F, 0, r + 1, t))
        smooth_row(r)
        return carry

    lax.fori_loop(2, rows - 2, inner_row, 0, unroll=2)
    for r in (0, 1, rows - 2):
        field_row(r, lambda t, r=r: whole(F, 0, r + 1, t))

    @pl.when(row > 0)
    def _():
        up.wait_recv()

    @pl.when(row < nrow - 1)
    def _():
        down.wait_recv()
        down_face.wait_recv()

    field_row(rows - 1, lambda t: jnp.concatenate([FN[spot(0, b, t), :] for b in range(blocks)], 0))
    for r in (0, 1, rows - 2, rows - 1):
        smooth_row(r)

    edge_copy(1, right).wait_recv()
    edge_copy(0, left).wait_recv()
    local = width <= cells
    from_left = jnp.where(local, EX[1], next_hi)
    from_right = jnp.where(local, EX[0], next_lo)

    def fixed(raw, edge, t):
        if t == 0:
            raw = jnp.where(low, edge, raw)
        if t == last:
            raw = jnp.where(high, edge, raw)
        return raw

    face_left.wait_recv()
    edge_f = unpack(from_right, fields - 1)
    for t in range(tiles):
        O[fields - 1, layer(0, cells - 1, t), :] = 0.5 * (F[nface - 1, layer(0, cells - 1, t), :] + fixed(RF[t], edge_f, t))

    for k in range(nvar):
        halo(1, right, k).wait_recv()
        halo(0, left, k).wait_recv()
        edge_l = unpack(from_left, k)
        edge_r = unpack(from_right, k)
        for t in range(tiles):
            scale = diffusion[k : k + 1, part(t)] * (1.0 / 12.0)
            l1 = fixed(R[1, k, 1, t], edge_l, t) - H[k, layer(2, cells - 1, t), :]
            l2 = fixed(R[1, k, 0, t], edge_l, t) - H[k, layer(2, cells - 2, t), :]
            r1 = fixed(R[0, k, 0, t], edge_r, t) - H[k, layer(2, 0, t), :]
            r2 = fixed(R[0, k, 1, t], edge_r, t) - H[k, layer(2, 1, t), :]
            for cell, term in ((0, 16.0 * l1 - l2), (1, -l1), (cells - 2, -r1), (cells - 1, 16.0 * r1 - r2)):
                O[k, layer(0, cell, t), :] = O[k, layer(0, cell, t), :] + scale * term

    for k in range(nvar):
        near_copy(k).wait_send()
        far_copy(k).wait_send()
    edge_copy(near_way, partner).wait_send()
    edge_copy(far_way, far).wait_send()
    face_left.wait_send()
    mean_near.wait_send()
    for step in range(1, pairs):
        mean_copy(step).wait_send()

    @pl.when(row > 0)
    def _():
        down.wait_send()
        down_face.wait_send()

    @pl.when(row < nrow - 1)
    def _():
        up.wait_send()


def spill(pieces, conserved, faces, conserved_out, faces_out, sem):
    fields = conserved.shape[0]
    size = conserved.shape[1] // pieces
    copies = []
    for k in range(fields + faces.shape[0]):
        source, target, i = (conserved, conserved_out, k) if k < fields else (faces, faces_out, k - fields)
        for p in range(pieces):
            where = pl.ds(p * size, size)
            copies.append(pltpu.make_async_copy(source.at[i, where], target.at[i, where], sem.at[k, p]))
    for c in copies:
        c.start()
    for c in copies:
        c.wait()


def blocked(x):
    n, rows, cells, theta = x.shape
    x = x.reshape(n, rows, cells // SUB, SUB, theta // LANES, LANES)
    return x.transpose(0, 1, 2, 4, 3, 5).reshape(n, rows * cells * (theta // LANES), LANES)


def unblocked(x, rows, cells, theta):
    x = x.reshape(x.shape[0], rows, cells // SUB, theta // LANES, SUB, LANES)
    return x.transpose(0, 1, 2, 4, 3, 5).reshape(x.shape[0], rows, cells, theta)


def body(nrow, nphi, hydro_vars, face_b, widths, diffusion):
    nvar, rows, cells, theta = hydro_vars.shape
    nface = face_b.shape[0]
    fields = nvar + nface
    cycles = widths.shape[0] // 2
    tiles = theta // LANES
    ring = cells * tiles
    f32 = jnp.float32
    shape = lambda *s: pltpu.VMEM(s, f32)
    far = pl.BlockSpec(memory_space=pltpu.HBM)
    near = pl.BlockSpec(memory_space=pltpu.VMEM)
    result_bytes = (fields + nface) * rows * ring * LANES * 4
    conserved, faces = pl.pallas_call(
        functools.partial(kernel, nrow, nphi, rows, cells, tiles, cycles),
        out_shape=(
            pltpu.VMEM((fields, rows * ring, LANES), f32),
            pltpu.VMEM((nface, rows * ring, LANES), f32),
        ),
        in_specs=[far, far, far, far],
        out_specs=(near, near),
        scratch_shapes=[
            shape(nvar, (rows + 4) * ring, LANES),
            shape(2, nvar, 2, tiles, rows, LANES),
            shape(2, nvar, 2, tiles, rows, LANES),
            shape(tiles, rows, LANES),
            shape(tiles, rows, LANES),
            shape(ring, LANES),
            shape(rows * cells, LANES),
            shape(rows, LANES),
            shape(rows, LANES),
            shape(rows, LANES),
            shape(nphi // 2, rows, LANES),
            shape(2, rows, LANES),
            shape(2, rows, LANES),
            pltpu.SMEM((2 * cycles,), jnp.int32),
            shape(nvar, theta),
            pltpu.SemaphoreType.DMA((2,)),
            pltpu.SemaphoreType.DMA((fields,)),
            pltpu.SemaphoreType.DMA((2, nvar)),
            pltpu.SemaphoreType.DMA((2, nvar)),
            pltpu.SemaphoreType.DMA((3,)),
            pltpu.SemaphoreType.DMA((3,)),
            pltpu.SemaphoreType.DMA((nphi // 2,)),
            pltpu.SemaphoreType.DMA((nphi // 2,)),
            pltpu.SemaphoreType.DMA((3,)),
            pltpu.SemaphoreType.DMA((3,)),
            pltpu.SemaphoreType.REGULAR((nphi // 2,)),
            pltpu.SemaphoreType.REGULAR,
            pltpu.SemaphoreType.REGULAR,
        ],
        compiler_params=pltpu.CompilerParams(
            collective_id=0, has_side_effects=True, vmem_limit_bytes=LIMIT - result_bytes
        ),
        name="step",
    )(widths, blocked(hydro_vars), blocked(face_b), diffusion)
    pieces = 2
    conserved, faces = pl.pallas_call(
        functools.partial(spill, pieces),
        out_shape=(
            jax.ShapeDtypeStruct((fields, rows * ring, LANES), f32),
            jax.ShapeDtypeStruct((nface, rows * ring, LANES), f32),
        ),
        in_specs=[near, near],
        out_specs=(far, far),
        scratch_shapes=[pltpu.SemaphoreType.DMA((fields + nface, pieces))],
        compiler_params=pltpu.CompilerParams(vmem_limit_bytes=1000000),
        name="spill",
    )(conserved, faces)
    return unblocked(conserved, rows, cells, theta), unblocked(faces, rows, cells, theta)


def solution(mesh):
    spec = P(None, "row", "phi", None)
    return jax.shard_map(
        functools.partial(body, mesh.shape["row"], mesh.shape["phi"]),
        mesh=mesh,
        in_specs=(spec, spec, P(), P()),
        out_specs=(spec, spec),
        check_vma=False,
    )
```

```python
import functools

import jax
import jax.numpy as jnp
from jax import lax
from jax.experimental import pallas as pl
from jax.experimental.pallas import tpu as pltpu
from jax.sharding import PartitionSpec as P

MESH = pl.DeviceIdType.MESH
LANES = 128
SUB = 8
EARLY = 1
MIDDLE = 2
LIMIT = 58000000


def kernel(
    nrow, nphi, rows, cells, tiles, cycles,
    widths_far, hydro, face, diffusion_far, O, F,
    H, S, R, SF, RF, FN, Q, M, PX, OM, MG, E, EX,
    widths, diffusion, small_sem, load_sem, send_phi, recv_phi, send_edge, recv_edge,
    send_mean, recv_mean, send_row, recv_row, pair_ack, far_ack, row_ack,
):
    nvar = hydro.shape[0]
    nface = face.shape[0]
    fields = nvar + nface
    last = tiles - 1
    blocks = cells // SUB
    ring = cells * tiles
    row = lax.axis_index("row")
    phi = lax.axis_index("phi")
    left = lax.rem(phi + nphi - 1, nphi)
    right = lax.rem(phi + 1, nphi)
    pairs = nphi // 2
    pair = phi // 2
    odd = lax.rem(phi, 2)
    partner = phi + 1 - 2 * odd
    far = jnp.where(odd == 1, right, left)
    near_way, far_way = 1 - odd, odd
    packed = 2 * cycles

    loads = [pltpu.make_async_copy(hydro.at[k], H.at[k, pl.ds(2 * ring, rows * ring)], load_sem.at[k]) for k in range(nvar)]
    loads += [pltpu.make_async_copy(face.at[k], F.at[k], load_sem.at[nvar + k]) for k in range(nface)]
    small = [
        pltpu.make_async_copy(widths_far, widths, small_sem.at[0]),
        pltpu.make_async_copy(diffusion_far, diffusion, small_sem.at[1]),
    ]
    for c in small + loads:
        c.start()

    barrier = pltpu.get_barrier_semaphore()

    def greet(**device):
        pl.semaphore_signal(barrier, inc=1, device_id=device, device_id_type=MESH)

    greet(phi=partner)

    @pl.when(far > phi)
    def _():
        greet(phi=far)

    @pl.when(row < nrow - 1)
    def _():
        greet(row=row + 1)

    for step in range(1, pairs):

        @pl.when(pair + step < pairs)
        def _(step=step):
            greet(phi=phi + 2 * step)

    lane = lax.broadcasted_iota(jnp.int32, (1, LANES), 1)
    low = lane < cycles
    high = lane >= LANES - cycles
    mine = [(lane >= packed * f) & (lane < packed * (f + 1)) for f in range(fields)]

    def part(t):
        return slice(t * LANES, (t + 1) * LANES)

    def pack(value, f):
        return pltpu.roll(value, (cycles + packed * f) % LANES, 1)

    def unpack(value, f):
        return pltpu.roll(value, (-(cycles + packed * f)) % LANES, 1)

    def spot(r, b, t):
        start = r * ring + (b * tiles + t) * SUB
        return pl.ds(start if isinstance(r, int) else pl.multiple_of(start, SUB), SUB)

    def layer(r, cell, t):
        return pl.ds(r * ring + (cell // SUB * tiles + t) * SUB + cell % SUB, rows, stride=ring)

    def place(f):
        return (H, f, 2) if f < nvar else (F, f - nvar, 0)

    def halo(way, target, k):
        return pltpu.make_async_remote_copy(
            src_ref=S.at[way, k], dst_ref=R.at[way, k], send_sem=send_phi.at[way, k], recv_sem=recv_phi.at[way, k],
            device_id={"phi": target}, device_id_type=MESH)

    def near_copy(k):
        return halo(near_way, partner, k)

    def far_copy(k):
        return halo(far_way, far, k)

    mean_near = pltpu.make_async_remote_copy(
        src_ref=M, dst_ref=PX, send_sem=send_mean.at[0], recv_sem=recv_mean.at[0],
        device_id={"phi": partner}, device_id_type=MESH)

    def mean_copy(step):
        return pltpu.make_async_remote_copy(
            src_ref=MG.at[pair], dst_ref=MG.at[pair], send_sem=send_mean.at[step], recv_sem=recv_mean.at[step],
            device_id={"phi": lax.rem(phi + 2 * step, nphi)}, device_id_type=MESH)

    def pack_halo(k):
        for t in range(tiles):
            for i in range(2):
                S[0, k, i, t] = H[k, layer(2, i, t), :]
                S[1, k, i, t] = H[k, layer(2, cells - 2 + i, t), :]

    for k in range(nvar):
        loads[k].wait()
        pack_halo(k)
        if k == 0:
            known = 1 + jnp.where(far < phi, 1, 0) + pair + jnp.where(row > 0, 1, 0)
            pl.semaphore_wait(barrier, known)
            for step in range(1, pairs):

                @pl.when(pair >= step)
                def _(step=step):
                    pl.semaphore_signal(pair_ack.at[step], inc=1, device_id={"phi": phi - 2 * step}, device_id_type=MESH)

            @pl.when(far < phi)
            def _():
                pl.semaphore_signal(far_ack, inc=1, device_id={"phi": far}, device_id_type=MESH)

            @pl.when(row > 0)
            def _():
                pl.semaphore_signal(row_ack, inc=1, device_id={"row": row - 1}, device_id_type=MESH)

        if k < EARLY:
            near_copy(k).start()
    for c in loads[nvar:]:
        c.wait()

    def polar_cells(r, b):
        value = jnp.zeros((SUB, LANES), jnp.float32)
        for f in range(fields):
            ref, k, base = place(f)
            polar = jnp.where(low, ref[k, spot(r + base, b, 0), :], ref[k, spot(r + base, b, last), :])
            value = jnp.where(mine[f], pack(polar, f), value)
        return value

    def cell_mean(r, carry):
        value = jnp.zeros((SUB, LANES), jnp.float32)
        for f in range(fields):
            ref, k, base = place(f)
            sums = [ref[k, spot(r + base, 0, t), :] for t in (0, last)]
            for b in range(1, blocks):
                sums = [x + ref[k, spot(r + base, b, t), :] for x, t in zip(sums, (0, last))]
            value = jnp.where(mine[f], pack(jnp.where(low, sums[0], sums[1]), f), value)
        size = SUB // 2
        while size:
            value = value + pltpu.roll(value, size, 0)
            size //= 2
        M[pl.ds(r, 1), :] = value[0:1] * (1.0 / cells)
        return carry

    lax.fori_loop(0, rows, cell_mean, 0, unroll=4)
    mean_near.start()
    for k in range(EARLY, MIDDLE):
        near_copy(k).start()
    for t in range(tiles):
        SF[t] = F[nface - 1, layer(0, 0, t), :]

    for c in small:
        c.wait()
    width = jnp.zeros((1, LANES), jnp.int32)
    slot = lax.rem(lane, packed)
    for j in range(cycles):
        width = jnp.where(slot == cycles + j, widths[j], width)
        width = jnp.where(slot == j, widths[cycles + j], width)

    index = lax.broadcasted_iota(jnp.int32, (SUB, LANES), 0)

    def local_average(r, carry):
        totals = [polar_cells(r, b) for b in range(blocks)]
        results = list(totals)
        size = 1
        while size < cells:
            if size < SUB:
                turned = []
                for v in totals:
                    forward = pltpu.roll(v, SUB - size, 0)
                    if 2 * size < SUB:
                        forward = jnp.where((index & size) == 0, forward, pltpu.roll(v, size, 0))
                    turned.append(v + forward)
                totals = turned
            else:
                hop = size // SUB
                totals = [totals[b] + totals[b ^ hop] for b in range(blocks)]
            size *= 2
            results = [jnp.where(width == size, v * (1.0 / size), old) for v, old in zip(totals, results)]
        for b in range(blocks):
            Q[pl.ds(pl.multiple_of(r * cells + b * SUB, SUB), SUB), :] = results[b]
        E[0, pl.ds(r, 1), :] = results[0][0:1]
        E[1, pl.ds(r, 1), :] = results[blocks - 1][SUB - 1 : SUB]
        return carry

    lax.fori_loop(0, rows, local_average, 0, unroll=2)

    def edge_copy(way, target):
        return pltpu.make_async_remote_copy(
            src_ref=E.at[way], dst_ref=EX.at[way], send_sem=send_edge.at[way], recv_sem=recv_edge.at[way],
            device_id={"phi": target}, device_id_type=MESH)

    face_left = pltpu.make_async_remote_copy(
        src_ref=SF, dst_ref=RF, send_sem=send_edge.at[2], recv_sem=recv_edge.at[2],
        device_id={"phi": left}, device_id_type=MESH)
    edge_copy(near_way, partner).start()

    @pl.when(odd == 1)
    def _():
        face_left.start()

    for k in range(MIDDLE, nvar):
        near_copy(k).start()

    mean_near.wait_recv()
    MG[pair] = (M[...] + PX[...]) * 0.5
    for step in range(1, pairs):

        @pl.when(pair + step < pairs)
        def _(step=step):
            pl.semaphore_wait(pair_ack.at[step], 1)

        mean_copy(step).start()

    def start_far():
        @pl.when(far > phi)
        def _():
            pl.semaphore_wait(far_ack, 1)

        edge_copy(far_way, far).start()

        @pl.when(odd == 0)
        def _():
            face_left.start()

        for k in range(nvar):
            far_copy(k).start()

    @pl.when(phi > 0)
    def _():
        start_far()

    for step in range(pairs - 1, 1, -1):
        mean_copy(step).wait_recv()

    @pl.when(phi == 0)
    def _():
        start_far()

    mean_copy(1).wait_recv()

    def group_mean(who):
        result = MG[who // 2]
        size = 2
        while size <= pairs:
            start = (who // (2 * size)) * size
            total = MG[start]
            for i in range(1, size):
                total = total + MG[start + i]
            result = jnp.where(width == 2 * size * cells, total * (1.0 / size), result)
            size *= 2
        return result

    OM[...] = group_mean(phi)
    next_lo = group_mean(right)
    next_hi = group_mean(left)
    wide = width > cells

    def spread(r):
        mean = jnp.broadcast_to(OM[pl.ds(r, 1), :], (SUB, LANES))
        for b in range(blocks):
            where = pl.ds(r * cells + b * SUB if isinstance(r, int) else pl.multiple_of(r * cells + b * SUB, SUB), SUB)
            value = jnp.where(wide, mean, Q[where, :])
            for f in range(fields):
                ref, k, base = place(f)
                polar = unpack(value, f)
                ref[k, spot(r + base, b, 0), :] = jnp.where(low, polar, ref[k, spot(r + base, b, 0), :])
                ref[k, spot(r + base, b, last), :] = jnp.where(high, polar, ref[k, spot(r + base, b, last), :])

    for r in (0, 1, rows - 2, rows - 1):
        spread(r)
    lax.fori_loop(2, rows - 2, lambda r, c: (spread(r), c)[1], 0, unroll=4)

    down = pltpu.make_async_remote_copy(
        src_ref=H.at[:, pl.ds(2 * ring, 2 * ring)], dst_ref=H.at[:, pl.ds((rows + 2) * ring, 2 * ring)],
        send_sem=send_row.at[0], recv_sem=recv_row.at[0], device_id={"row": row - 1}, device_id_type=MESH)
    down_face = pltpu.make_async_remote_copy(
        src_ref=F.at[0, pl.ds(0, ring)], dst_ref=FN,
        send_sem=send_row.at[1], recv_sem=recv_row.at[1], device_id={"row": row - 1}, device_id_type=MESH)
    up = pltpu.make_async_remote_copy(
        src_ref=H.at[:, pl.ds(rows * ring, 2 * ring)], dst_ref=H.at[:, pl.ds(0, 2 * ring)],
        send_sem=send_row.at[2], recv_sem=recv_row.at[2], device_id={"row": row + 1}, device_id_type=MESH)

    @pl.when(row > 0)
    def _():
        down.start()
        down_face.start()

    @pl.when(row < nrow - 1)
    def _():
        pl.semaphore_wait(row_ack, 1)
        up.start()

    @pl.when(row == 0)
    def _():
        H[:, pl.ds(0, 2 * ring), :] = jnp.zeros((nvar, 2 * ring, LANES), jnp.float32)

    @pl.when(row == nrow - 1)
    def _():
        H[:, pl.ds((rows + 2) * ring, 2 * ring), :] = jnp.zeros((nvar, 2 * ring, LANES), jnp.float32)
        FN[...] = jnp.zeros_like(FN)

    def whole(ref, k, r, t):
        return jnp.concatenate([ref[k, spot(r, b, t), :] for b in range(blocks)], 0)

    def write(k, r, t, value):
        for b in range(blocks):
            O[k, spot(r, b, t), :] = value[b * SUB : (b + 1) * SUB]

    def shifted(parts, amount):
        out = []
        turned = [pltpu.roll(p, (-amount) % LANES, 1) for p in parts]
        for t in range(tiles):
            if amount > 0:
                inside = lane < LANES - amount
                other = turned[t + 1] if t + 1 < tiles else 0.0
            else:
                inside = lane >= -amount
                other = turned[t - 1] if t > 0 else 0.0
            out.append(jnp.where(inside, turned[t], other))
        return out

    def smooth_row(r):
        for k in range(nvar):
            mid = [whole(H, k, r + 2, t) for t in range(tiles)]
            one = [a + b for a, b in zip(shifted(mid, 1), shifted(mid, -1))]
            two = [a + b for a, b in zip(shifted(mid, 2), shifted(mid, -2))]
            for t in range(tiles):
                v = mid[t]
                s1 = one[t] + (pltpu.roll(v, 1, 0) + pltpu.roll(v, cells - 1, 0)) + (whole(H, k, r + 1, t) + whole(H, k, r + 3, t))
                s2 = two[t] + (pltpu.roll(v, 2, 0) + pltpu.roll(v, cells - 2, 0)) + (whole(H, k, r, t) + whole(H, k, r + 4, t))
                change = (16.0 * s1 - s2 - 90.0 * v) * (1.0 / 12.0)
                write(k, r, t, v + diffusion[k : k + 1, part(t)] * change)

    def field_row(r, following):
        polar = [whole(F, 1, r, t) for t in range(tiles)]
        polar_next = shifted(polar, 1)
        for t in range(tiles):
            write(nvar, r, t, 0.5 * (whole(F, 0, r, t) + following(t)))
            write(nvar + 1, r, t, 0.5 * (polar[t] + polar_next[t]))
            azimuth = whole(F, 2, r, t)
            write(nvar + 2, r, t, 0.5 * (azimuth + pltpu.roll(azimuth, cells - 1, 0)))

    def inner_row(r, carry):
        field_row(r, lambda t: whole(F, 0, r + 1, t))
        smooth_row(r)
        return carry

    lax.fori_loop(2, rows - 2, inner_row, 0, unroll=2)
    for r in (0, 1, rows - 2):
        field_row(r, lambda t, r=r: whole(F, 0, r + 1, t))

    @pl.when(row > 0)
    def _():
        up.wait_recv()

    @pl.when(row < nrow - 1)
    def _():
        down.wait_recv()
        down_face.wait_recv()

    field_row(rows - 1, lambda t: jnp.concatenate([FN[spot(0, b, t), :] for b in range(blocks)], 0))
    for r in (0, 1, rows - 2, rows - 1):
        smooth_row(r)

    edge_copy(1, right).wait_recv()
    edge_copy(0, left).wait_recv()
    local = width <= cells
    from_left = jnp.where(local, EX[1], next_hi)
    from_right = jnp.where(local, EX[0], next_lo)

    def fixed(raw, edge, t):
        if t == 0:
            raw = jnp.where(low, edge, raw)
        if t == last:
            raw = jnp.where(high, edge, raw)
        return raw

    face_left.wait_recv()
    edge_f = unpack(from_right, fields - 1)
    for t in range(tiles):
        O[fields - 1, layer(0, cells - 1, t), :] = 0.5 * (F[nface - 1, layer(0, cells - 1, t), :] + fixed(RF[t], edge_f, t))

    for k in range(nvar):
        halo(1, right, k).wait_recv()
        halo(0, left, k).wait_recv()
        edge_l = unpack(from_left, k)
        edge_r = unpack(from_right, k)
        for t in range(tiles):
            scale = diffusion[k : k + 1, part(t)] * (1.0 / 12.0)
            l1 = fixed(R[1, k, 1, t], edge_l, t) - H[k, layer(2, cells - 1, t), :]
            l2 = fixed(R[1, k, 0, t], edge_l, t) - H[k, layer(2, cells - 2, t), :]
            r1 = fixed(R[0, k, 0, t], edge_r, t) - H[k, layer(2, 0, t), :]
            r2 = fixed(R[0, k, 1, t], edge_r, t) - H[k, layer(2, 1, t), :]
            for cell, term in ((0, 16.0 * l1 - l2), (1, -l1), (cells - 2, -r1), (cells - 1, 16.0 * r1 - r2)):
                O[k, layer(0, cell, t), :] = O[k, layer(0, cell, t), :] + scale * term

    for k in range(nvar):
        near_copy(k).wait_send()
        far_copy(k).wait_send()
    edge_copy(near_way, partner).wait_send()
    edge_copy(far_way, far).wait_send()
    face_left.wait_send()
    mean_near.wait_send()
    for step in range(1, pairs):
        mean_copy(step).wait_send()

    @pl.when(row > 0)
    def _():
        down.wait_send()
        down_face.wait_send()

    @pl.when(row < nrow - 1)
    def _():
        up.wait_send()


def spill(pieces, conserved, faces, conserved_out, faces_out, sem):
    fields = conserved.shape[0]
    size = conserved.shape[1] // pieces
    copies = []
    for k in range(fields + faces.shape[0]):
        source, target, i = (conserved, conserved_out, k) if k < fields else (faces, faces_out, k - fields)
        for p in range(pieces):
            where = pl.ds(p * size, size)
            copies.append(pltpu.make_async_copy(source.at[i, where], target.at[i, where], sem.at[k, p]))
    for c in copies:
        c.start()
    for c in copies:
        c.wait()


def blocked(x):
    n, rows, cells, theta = x.shape
    x = x.reshape(n, rows, cells // SUB, SUB, theta // LANES, LANES)
    return x.transpose(0, 1, 2, 4, 3, 5).reshape(n, rows * cells * (theta // LANES), LANES)


def unblocked(x, rows, cells, theta):
    x = x.reshape(x.shape[0], rows, cells // SUB, theta // LANES, SUB, LANES)
    return x.transpose(0, 1, 2, 4, 3, 5).reshape(x.shape[0], rows, cells, theta)


def body(nrow, nphi, hydro_vars, face_b, widths, diffusion):
    nvar, rows, cells, theta = hydro_vars.shape
    nface = face_b.shape[0]
    fields = nvar + nface
    cycles = widths.shape[0] // 2
    tiles = theta // LANES
    ring = cells * tiles
    f32 = jnp.float32
    shape = lambda *s: pltpu.VMEM(s, f32)
    far = pl.BlockSpec(memory_space=pltpu.HBM)
    near = pl.BlockSpec(memory_space=pltpu.VMEM)
    result_bytes = (fields + nface) * rows * ring * LANES * 4
    conserved, faces = pl.pallas_call(
        functools.partial(kernel, nrow, nphi, rows, cells, tiles, cycles),
        out_shape=(
            pltpu.VMEM((fields, rows * ring, LANES), f32),
            pltpu.VMEM((nface, rows * ring, LANES), f32),
        ),
        in_specs=[far, far, far, far],
        out_specs=(near, near),
        scratch_shapes=[
            shape(nvar, (rows + 4) * ring, LANES),
            shape(2, nvar, 2, tiles, rows, LANES),
            shape(2, nvar, 2, tiles, rows, LANES),
            shape(tiles, rows, LANES),
            shape(tiles, rows, LANES),
            shape(ring, LANES),
            shape(rows * cells, LANES),
            shape(rows, LANES),
            shape(rows, LANES),
            shape(rows, LANES),
            shape(nphi // 2, rows, LANES),
            shape(2, rows, LANES),
            shape(2, rows, LANES),
            pltpu.SMEM((2 * cycles,), jnp.int32),
            shape(nvar, theta),
            pltpu.SemaphoreType.DMA((2,)),
            pltpu.SemaphoreType.DMA((fields,)),
            pltpu.SemaphoreType.DMA((2, nvar)),
            pltpu.SemaphoreType.DMA((2, nvar)),
            pltpu.SemaphoreType.DMA((3,)),
            pltpu.SemaphoreType.DMA((3,)),
            pltpu.SemaphoreType.DMA((nphi // 2,)),
            pltpu.SemaphoreType.DMA((nphi // 2,)),
            pltpu.SemaphoreType.DMA((3,)),
            pltpu.SemaphoreType.DMA((3,)),
            pltpu.SemaphoreType.REGULAR((nphi // 2,)),
            pltpu.SemaphoreType.REGULAR,
            pltpu.SemaphoreType.REGULAR,
        ],
        compiler_params=pltpu.CompilerParams(
            collective_id=0, has_side_effects=True, vmem_limit_bytes=LIMIT - result_bytes
        ),
        name="step",
    )(widths, blocked(hydro_vars), blocked(face_b), diffusion)
    pieces = 2
    conserved, faces = pl.pallas_call(
        functools.partial(spill, pieces),
        out_shape=(
            jax.ShapeDtypeStruct((fields, rows * ring, LANES), f32),
            jax.ShapeDtypeStruct((nface, rows * ring, LANES), f32),
        ),
        in_specs=[near, near],
        out_specs=(far, far),
        scratch_shapes=[pltpu.SemaphoreType.DMA((fields + nface, pieces))],
        compiler_params=pltpu.CompilerParams(vmem_limit_bytes=1000000),
        name="spill",
    )(conserved, faces)
    return unblocked(conserved, rows, cells, theta), unblocked(faces, rows, cells, theta)


def solution(mesh):
    spec = P(None, "row", "phi", None)
    return jax.shard_map(
        functools.partial(body, mesh.shape["row"], mesh.shape["phi"]),
        mesh=mesh,
        in_specs=(spec, spec, P(), P()),
        out_specs=(spec, spec),
        check_vma=False,
    )
```

```python
import functools

import jax
import jax.numpy as jnp
from jax import lax
from jax.experimental import pallas as pl
from jax.experimental.pallas import tpu as pltpu
from jax.sharding import PartitionSpec as P

MESH = pl.DeviceIdType.MESH
LANES = 128
SUB = 8
EARLY = 1
MIDDLE = 2
LIMIT = 58000000


def kernel(
    nrow, nphi, rows, cells, tiles, cycles,
    widths_far, hydro, face, diffusion_far, O, F,
    H, S, R, SF, RF, FN, Q, M, PX, OM, MG, E,
    widths, diffusion, small_sem, load_sem, send_phi, recv_phi, send_face, recv_face,
    send_mean, recv_mean, send_row, recv_row, pair_ack, far_ack, row_ack,
):
    nvar = hydro.shape[0]
    nface = face.shape[0]
    fields = nvar + nface
    last = tiles - 1
    blocks = cells // SUB
    ring = cells * tiles
    row = lax.axis_index("row")
    phi = lax.axis_index("phi")
    left = lax.rem(phi + nphi - 1, nphi)
    right = lax.rem(phi + 1, nphi)
    pairs = nphi // 2
    pair = phi // 2
    odd = lax.rem(phi, 2)
    partner = phi + 1 - 2 * odd
    far = jnp.where(odd == 1, right, left)
    near_way, far_way = 1 - odd, odd
    packed = 2 * cycles

    loads = [pltpu.make_async_copy(hydro.at[k], H.at[k, pl.ds(2 * ring, rows * ring)], load_sem.at[k]) for k in range(nvar)]
    loads += [pltpu.make_async_copy(face.at[k], F.at[k], load_sem.at[nvar + k]) for k in range(nface)]
    small = [
        pltpu.make_async_copy(widths_far, widths, small_sem.at[0]),
        pltpu.make_async_copy(diffusion_far, diffusion, small_sem.at[1]),
    ]
    for c in small + loads:
        c.start()

    barrier = pltpu.get_barrier_semaphore()

    def greet(**device):
        pl.semaphore_signal(barrier, inc=1, device_id=device, device_id_type=MESH)

    greet(phi=partner)

    @pl.when(far > phi)
    def _():
        greet(phi=far)

    @pl.when(row < nrow - 1)
    def _():
        greet(row=row + 1)

    for step in range(1, pairs):

        @pl.when(pair + step < pairs)
        def _(step=step):
            greet(phi=phi + 2 * step)

    lane = lax.broadcasted_iota(jnp.int32, (1, LANES), 1)
    low = lane < cycles
    high = lane >= LANES - cycles
    mine = [(lane >= packed * f) & (lane < packed * (f + 1)) for f in range(fields)]

    def part(t):
        return slice(t * LANES, (t + 1) * LANES)

    def pack(value, f):
        return pltpu.roll(value, (cycles + packed * f) % LANES, 1)

    def unpack(value, f):
        return pltpu.roll(value, (-(cycles + packed * f)) % LANES, 1)

    def spot(r, b, t):
        start = r * ring + (b * tiles + t) * SUB
        return pl.ds(start if isinstance(r, int) else pl.multiple_of(start, SUB), SUB)

    def layer(r, cell, t):
        return pl.ds(r * ring + (cell // SUB * tiles + t) * SUB + cell % SUB, rows, stride=ring)

    def place(f):
        return (H, f, 2) if f < nvar else (F, f - nvar, 0)

    def halo(way, target, k):
        return pltpu.make_async_remote_copy(
            src_ref=S.at[way, k], dst_ref=R.at[way, k], send_sem=send_phi.at[way, k], recv_sem=recv_phi.at[way, k],
            device_id={"phi": target}, device_id_type=MESH)

    def near_copy(k):
        return halo(near_way, partner, k)

    def far_copy(k):
        return halo(far_way, far, k)

    mean_near = pltpu.make_async_remote_copy(
        src_ref=M, dst_ref=PX, send_sem=send_mean.at[0], recv_sem=recv_mean.at[0],
        device_id={"phi": partner}, device_id_type=MESH)

    def mean_copy(step):
        return pltpu.make_async_remote_copy(
            src_ref=MG.at[pair], dst_ref=MG.at[pair], send_sem=send_mean.at[step], recv_sem=recv_mean.at[step],
            device_id={"phi": lax.rem(phi + 2 * step, nphi)}, device_id_type=MESH)

    def pack_halo(k):
        for t in range(tiles):
            for i in range(2):
                S[0, k, i, t] = H[k, layer(2, i, t), :]
                S[1, k, i, t] = H[k, layer(2, cells - 2 + i, t), :]

    for k in range(nvar):
        loads[k].wait()
        pack_halo(k)
        if k == 0:
            known = 1 + jnp.where(far < phi, 1, 0) + pair + jnp.where(row > 0, 1, 0)
            pl.semaphore_wait(barrier, known)
            for step in range(1, pairs):

                @pl.when(pair >= step)
                def _(step=step):
                    pl.semaphore_signal(pair_ack.at[step], inc=1, device_id={"phi": phi - 2 * step}, device_id_type=MESH)

            @pl.when(far < phi)
            def _():
                pl.semaphore_signal(far_ack, inc=1, device_id={"phi": far}, device_id_type=MESH)

            @pl.when(row > 0)
            def _():
                pl.semaphore_signal(row_ack, inc=1, device_id={"row": row - 1}, device_id_type=MESH)

        if k < EARLY:
            near_copy(k).start()
    for c in loads[nvar:]:
        c.wait()
    face_left = pltpu.make_async_remote_copy(
        src_ref=SF, dst_ref=RF, send_sem=send_face, recv_sem=recv_face,
        device_id={"phi": left}, device_id_type=MESH)
    for t in range(tiles):
        SF[t] = F[nface - 1, layer(0, 0, t), :]

    @pl.when(odd == 1)
    def _():
        face_left.start()


    def polar_cells(r, b):
        value = jnp.zeros((SUB, LANES), jnp.float32)
        for f in range(fields):
            ref, k, base = place(f)
            polar = jnp.where(low, ref[k, spot(r + base, b, 0), :], ref[k, spot(r + base, b, last), :])
            value = jnp.where(mine[f], pack(polar, f), value)
        return value

    def cell_mean(r, carry):
        value = jnp.zeros((SUB, LANES), jnp.float32)
        for f in range(fields):
            ref, k, base = place(f)
            sums = [ref[k, spot(r + base, 0, t), :] for t in (0, last)]
            for b in range(1, blocks):
                sums = [x + ref[k, spot(r + base, b, t), :] for x, t in zip(sums, (0, last))]
            value = jnp.where(mine[f], pack(jnp.where(low, sums[0], sums[1]), f), value)
        size = SUB // 2
        while size:
            value = value + pltpu.roll(value, size, 0)
            size //= 2
        M[pl.ds(r, 1), :] = value[0:1] * (1.0 / cells)
        return carry

    lax.fori_loop(0, rows, cell_mean, 0, unroll=4)
    mean_near.start()
    for k in range(EARLY, MIDDLE):
        near_copy(k).start()

    for c in small:
        c.wait()
    width = jnp.zeros((1, LANES), jnp.int32)
    slot = lax.rem(lane, packed)
    for j in range(cycles):
        width = jnp.where(slot == cycles + j, widths[j], width)
        width = jnp.where(slot == j, widths[cycles + j], width)

    index = lax.broadcasted_iota(jnp.int32, (SUB, LANES), 0)

    def local_average(r, carry):
        totals = [polar_cells(r, b) for b in range(blocks)]
        results = list(totals)
        size = 1
        while size < cells:
            if size < SUB:
                turned = []
                for v in totals:
                    forward = pltpu.roll(v, SUB - size, 0)
                    if 2 * size < SUB:
                        forward = jnp.where((index & size) == 0, forward, pltpu.roll(v, size, 0))
                    turned.append(v + forward)
                totals = turned
            else:
                hop = size // SUB
                totals = [totals[b] + totals[b ^ hop] for b in range(blocks)]
            size *= 2
            results = [jnp.where(width == size, v * (1.0 / size), old) for v, old in zip(totals, results)]
        for b in range(blocks):
            Q[pl.ds(pl.multiple_of(r * cells + b * SUB, SUB), SUB), :] = results[b]
        E[0, pl.ds(r, 1), :] = results[0][0:1]
        E[1, pl.ds(r, 1), :] = results[blocks - 1][SUB - 1 : SUB]
        return carry

    lax.fori_loop(0, rows, local_average, 0, unroll=2)

    def put_edges(way, k, i, f, source):
        edges = unpack(E[source], f)
        S[way, k, i, 0] = jnp.where(low, edges, S[way, k, i, 0])
        S[way, k, i, last] = jnp.where(high, edges, S[way, k, i, last])

    for k in range(MIDDLE, nvar):
        for way in range(2):
            put_edges(way, k, 0, k, way)
    for k in range(MIDDLE):
        put_edges(far_way, k, 0, k, far_way)
        put_edges(near_way, k + MIDDLE, 1, k, near_way)
    put_edges(0, nvar - 1, 1, fields - 1, 0)

    for k in range(MIDDLE, nvar):
        near_copy(k).start()

    mean_near.wait_recv()
    MG[pair] = (M[...] + PX[...]) * 0.5
    for step in range(1, pairs):

        @pl.when(pair + step < pairs)
        def _(step=step):
            pl.semaphore_wait(pair_ack.at[step], 1)

        mean_copy(step).start()

    def start_far():
        @pl.when(far > phi)
        def _():
            pl.semaphore_wait(far_ack, 1)

        @pl.when(odd == 0)
        def _():
            edges = unpack(E[0], fields - 1)
            SF[0] = jnp.where(low, edges, SF[0])
            SF[last] = jnp.where(high, edges, SF[last])
            face_left.start()

        for k in range(nvar):
            far_copy(k).start()

    @pl.when(phi > 0)
    def _():
        start_far()

    for step in range(pairs - 1, 1, -1):
        mean_copy(step).wait_recv()

    @pl.when(phi == 0)
    def _():
        start_far()

    mean_copy(1).wait_recv()

    def group_mean(who):
        result = MG[who // 2]
        size = 2
        while size <= pairs:
            start = (who // (2 * size)) * size
            total = MG[start]
            for i in range(1, size):
                total = total + MG[start + i]
            result = jnp.where(width == 2 * size * cells, total * (1.0 / size), result)
            size *= 2
        return result

    OM[...] = group_mean(phi)
    next_lo = group_mean(right)
    next_hi = group_mean(left)
    wide = width > cells

    def spread(r):
        mean = jnp.broadcast_to(OM[pl.ds(r, 1), :], (SUB, LANES))
        for b in range(blocks):
            where = pl.ds(r * cells + b * SUB if isinstance(r, int) else pl.multiple_of(r * cells + b * SUB, SUB), SUB)
            value = jnp.where(wide, mean, Q[where, :])
            for f in range(fields):
                ref, k, base = place(f)
                polar = unpack(value, f)
                ref[k, spot(r + base, b, 0), :] = jnp.where(low, polar, ref[k, spot(r + base, b, 0), :])
                ref[k, spot(r + base, b, last), :] = jnp.where(high, polar, ref[k, spot(r + base, b, last), :])

    for r in (0, 1, rows - 2, rows - 1):
        spread(r)

    down = pltpu.make_async_remote_copy(
        src_ref=H.at[:, pl.ds(2 * ring, 2 * ring)], dst_ref=H.at[:, pl.ds((rows + 2) * ring, 2 * ring)],
        send_sem=send_row.at[0], recv_sem=recv_row.at[0], device_id={"row": row - 1}, device_id_type=MESH)
    down_face = pltpu.make_async_remote_copy(
        src_ref=F.at[0, pl.ds(0, ring)], dst_ref=FN,
        send_sem=send_row.at[1], recv_sem=recv_row.at[1], device_id={"row": row - 1}, device_id_type=MESH)
    up = pltpu.make_async_remote_copy(
        src_ref=H.at[:, pl.ds(rows * ring, 2 * ring)], dst_ref=H.at[:, pl.ds(0, 2 * ring)],
        send_sem=send_row.at[2], recv_sem=recv_row.at[2], device_id={"row": row + 1}, device_id_type=MESH)

    @pl.when(row > 0)
    def _():
        down.start()
        down_face.start()

    @pl.when(row < nrow - 1)
    def _():
        pl.semaphore_wait(row_ack, 1)
        up.start()

    lax.fori_loop(2, rows - 2, lambda r, c: (spread(r), c)[1], 0, unroll=4)

    @pl.when(row == 0)
    def _():
        H[:, pl.ds(0, 2 * ring), :] = jnp.zeros((nvar, 2 * ring, LANES), jnp.float32)

    @pl.when(row == nrow - 1)
    def _():
        H[:, pl.ds((rows + 2) * ring, 2 * ring), :] = jnp.zeros((nvar, 2 * ring, LANES), jnp.float32)
        FN[...] = jnp.zeros_like(FN)

    def whole(ref, k, r, t):
        return jnp.concatenate([ref[k, spot(r, b, t), :] for b in range(blocks)], 0)

    def write(k, r, t, value):
        for b in range(blocks):
            O[k, spot(r, b, t), :] = value[b * SUB : (b + 1) * SUB]

    def shifted(parts, amount):
        out = []
        turned = [pltpu.roll(p, (-amount) % LANES, 1) for p in parts]
        for t in range(tiles):
            if amount > 0:
                inside = lane < LANES - amount
                other = turned[t + 1] if t + 1 < tiles else 0.0
            else:
                inside = lane >= -amount
                other = turned[t - 1] if t > 0 else 0.0
            out.append(jnp.where(inside, turned[t], other))
        return out

    def smooth_row(r):
        for k in range(nvar):
            mid = [whole(H, k, r + 2, t) for t in range(tiles)]
            one = [a + b for a, b in zip(shifted(mid, 1), shifted(mid, -1))]
            two = [a + b for a, b in zip(shifted(mid, 2), shifted(mid, -2))]
            for t in range(tiles):
                v = mid[t]
                s1 = one[t] + (pltpu.roll(v, 1, 0) + pltpu.roll(v, cells - 1, 0)) + (whole(H, k, r + 1, t) + whole(H, k, r + 3, t))
                s2 = two[t] + (pltpu.roll(v, 2, 0) + pltpu.roll(v, cells - 2, 0)) + (whole(H, k, r, t) + whole(H, k, r + 4, t))
                change = (16.0 * s1 - s2 - 90.0 * v) * (1.0 / 12.0)
                write(k, r, t, v + diffusion[k : k + 1, part(t)] * change)

    def field_row(r, following):
        polar = [whole(F, 1, r, t) for t in range(tiles)]
        polar_next = shifted(polar, 1)
        for t in range(tiles):
            write(nvar, r, t, 0.5 * (whole(F, 0, r, t) + following(t)))
            write(nvar + 1, r, t, 0.5 * (polar[t] + polar_next[t]))
            azimuth = whole(F, 2, r, t)
            write(nvar + 2, r, t, 0.5 * (azimuth + pltpu.roll(azimuth, cells - 1, 0)))

    def inner_row(r, carry):
        field_row(r, lambda t: whole(F, 0, r + 1, t))
        smooth_row(r)
        return carry

    lax.fori_loop(2, rows - 2, inner_row, 0, unroll=2)
    for r in (0, 1, rows - 2):
        field_row(r, lambda t, r=r: whole(F, 0, r + 1, t))

    @pl.when(row > 0)
    def _():
        up.wait_recv()

    @pl.when(row < nrow - 1)
    def _():
        down.wait_recv()
        down_face.wait_recv()

    field_row(rows - 1, lambda t: jnp.concatenate([FN[spot(0, b, t), :] for b in range(blocks)], 0))
    for r in (0, 1, rows - 2, rows - 1):
        smooth_row(r)

    local = unpack(width, 0) <= cells

    def fixed(raw, edge, t):
        if t == 0:
            raw = jnp.where(low, edge, raw)
        if t == last:
            raw = jnp.where(high, edge, raw)
        return raw

    def sent_edge(way, k, t):
        if k >= MIDDLE:
            return R[way, k, 0, t]
        return jnp.where(odd == way, R[way, k + MIDDLE, 1, t], R[way, k, 0, t])

    def patch(k):
        mean_l = unpack(next_hi, k)
        mean_r = unpack(next_lo, k)
        for t in range(tiles):
            scale = diffusion[k : k + 1, part(t)] * (1.0 / 12.0)
            edge_l = jnp.where(local, sent_edge(1, k, t), mean_l)
            edge_r = jnp.where(local, sent_edge(0, k, t), mean_r)
            l1 = fixed(R[1, k, 1, t], edge_l, t) - H[k, layer(2, cells - 1, t), :]
            l2 = fixed(R[1, k, 0, t], edge_l, t) - H[k, layer(2, cells - 2, t), :]
            r1 = fixed(R[0, k, 0, t], edge_r, t) - H[k, layer(2, 0, t), :]
            r2 = fixed(R[0, k, 1, t], edge_r, t) - H[k, layer(2, 1, t), :]
            for cell, term in ((0, 16.0 * l1 - l2), (1, -l1), (cells - 2, -r1), (cells - 1, 16.0 * r1 - r2)):
                O[k, layer(0, cell, t), :] = O[k, layer(0, cell, t), :] + scale * term

    def arrive(k):
        halo(1, right, k).wait_recv()
        halo(0, left, k).wait_recv()

    for k in range(MIDDLE):
        arrive(k)
    face_left.wait_recv()
    for k in range(MIDDLE, nvar):
        arrive(k)
        if k < 2 * MIDDLE:
            patch(k - MIDDLE)
        patch(k)
    mean_f = unpack(next_lo, fields - 1)
    for t in range(tiles):
        edge_f = jnp.where(local, jnp.where(odd == 0, R[0, nvar - 1, 1, t], RF[t]), mean_f)
        O[fields - 1, layer(0, cells - 1, t), :] = 0.5 * (F[nface - 1, layer(0, cells - 1, t), :] + fixed(RF[t], edge_f, t))

    for k in range(nvar):
        near_copy(k).wait_send()
        far_copy(k).wait_send()
    face_left.wait_send()
    mean_near.wait_send()
    for step in range(1, pairs):
        mean_copy(step).wait_send()

    @pl.when(row > 0)
    def _():
        down.wait_send()
        down_face.wait_send()

    @pl.when(row < nrow - 1)
    def _():
        up.wait_send()


def spill(pieces, conserved, faces, conserved_out, faces_out, sem):
    fields = conserved.shape[0]
    size = conserved.shape[1] // pieces
    copies = []
    for k in range(fields + faces.shape[0]):
        source, target, i = (conserved, conserved_out, k) if k < fields else (faces, faces_out, k - fields)
        for p in range(pieces):
            where = pl.ds(p * size, size)
            copies.append(pltpu.make_async_copy(source.at[i, where], target.at[i, where], sem.at[k, p]))
    for c in copies:
        c.start()
    for c in copies:
        c.wait()


def blocked(x):
    n, rows, cells, theta = x.shape
    x = x.reshape(n, rows, cells // SUB, SUB, theta // LANES, LANES)
    return x.transpose(0, 1, 2, 4, 3, 5).reshape(n, rows * cells * (theta // LANES), LANES)


def unblocked(x, rows, cells, theta):
    x = x.reshape(x.shape[0], rows, cells // SUB, theta // LANES, SUB, LANES)
    return x.transpose(0, 1, 2, 4, 3, 5).reshape(x.shape[0], rows, cells, theta)


def body(nrow, nphi, hydro_vars, face_b, widths, diffusion):
    nvar, rows, cells, theta = hydro_vars.shape
    nface = face_b.shape[0]
    fields = nvar + nface
    cycles = widths.shape[0] // 2
    tiles = theta // LANES
    ring = cells * tiles
    f32 = jnp.float32
    shape = lambda *s: pltpu.VMEM(s, f32)
    far = pl.BlockSpec(memory_space=pltpu.HBM)
    near = pl.BlockSpec(memory_space=pltpu.VMEM)
    result_bytes = (fields + nface) * rows * ring * LANES * 4
    conserved, faces = pl.pallas_call(
        functools.partial(kernel, nrow, nphi, rows, cells, tiles, cycles),
        out_shape=(
            pltpu.VMEM((fields, rows * ring, LANES), f32),
            pltpu.VMEM((nface, rows * ring, LANES), f32),
        ),
        in_specs=[far, far, far, far],
        out_specs=(near, near),
        scratch_shapes=[
            shape(nvar, (rows + 4) * ring, LANES),
            shape(2, nvar, 2, tiles, rows, LANES),
            shape(2, nvar, 2, tiles, rows, LANES),
            shape(tiles, rows, LANES),
            shape(tiles, rows, LANES),
            shape(ring, LANES),
            shape(rows * cells, LANES),
            shape(rows, LANES),
            shape(rows, LANES),
            shape(rows, LANES),
            shape(nphi // 2, rows, LANES),
            shape(2, rows, LANES),
            pltpu.SMEM((2 * cycles,), jnp.int32),
            shape(nvar, theta),
            pltpu.SemaphoreType.DMA((2,)),
            pltpu.SemaphoreType.DMA((fields,)),
            pltpu.SemaphoreType.DMA((2, nvar)),
            pltpu.SemaphoreType.DMA((2, nvar)),
            pltpu.SemaphoreType.DMA,
            pltpu.SemaphoreType.DMA,
            pltpu.SemaphoreType.DMA((nphi // 2,)),
            pltpu.SemaphoreType.DMA((nphi // 2,)),
            pltpu.SemaphoreType.DMA((3,)),
            pltpu.SemaphoreType.DMA((3,)),
            pltpu.SemaphoreType.REGULAR((nphi // 2,)),
            pltpu.SemaphoreType.REGULAR,
            pltpu.SemaphoreType.REGULAR,
        ],
        compiler_params=pltpu.CompilerParams(
            collective_id=0, has_side_effects=True, vmem_limit_bytes=LIMIT - result_bytes
        ),
        name="step",
    )(widths, blocked(hydro_vars), blocked(face_b), diffusion)
    pieces = 1
    conserved, faces = pl.pallas_call(
        functools.partial(spill, pieces),
        out_shape=(
            jax.ShapeDtypeStruct((fields, rows * ring, LANES), f32),
            jax.ShapeDtypeStruct((nface, rows * ring, LANES), f32),
        ),
        in_specs=[near, near],
        out_specs=(far, far),
        scratch_shapes=[pltpu.SemaphoreType.DMA((fields + nface, pieces))],
        compiler_params=pltpu.CompilerParams(vmem_limit_bytes=1000000),
        name="spill",
    )(conserved, faces)
    return unblocked(conserved, rows, cells, theta), unblocked(faces, rows, cells, theta)


def solution(mesh):
    spec = P(None, "row", "phi", None)
    return jax.shard_map(
        functools.partial(body, mesh.shape["row"], mesh.shape["phi"]),
        mesh=mesh,
        in_specs=(spec, spec, P(), P()),
        out_specs=(spec, spec),
        check_vma=False,
    )
```

```python
import functools

import jax
import jax.numpy as jnp
from jax import lax
from jax.experimental import pallas as pl
from jax.experimental.pallas import tpu as pltpu
from jax.sharding import PartitionSpec as P

MESH = pl.DeviceIdType.MESH
LANES = 128
SUB = 8
EARLY = 1
MIDDLE = 2
LIMIT = 58000000


def late_slots(tiles):
    names = ["halo", "inner", "face", "face_edge", "scale"]
    sizes = [4 * tiles, 4 * tiles, tiles, tiles, tiles]
    starts, total = {}, 0
    for name, size in zip(names, sizes):
        starts[name] = total
        total += size
    for name in ("mean_left", "mean_right", "mean_face", "local"):
        starts[name] = total
        total += 1
    return starts, total


def fix_polar(low, high, last, raw, edge, t):
    if t == 0:
        raw = jnp.where(low, edge, raw)
    if t == last:
        raw = jnp.where(high, edge, raw)
    return raw


def halo_terms(scale, from_left, from_right, inner):
    l1, l2 = from_left[1] - inner[3], from_left[0] - inner[2]
    r1, r2 = from_right[0] - inner[0], from_right[1] - inner[1]
    return [scale * term for term in (16.0 * l1 - l2, -l1, -r1, 16.0 * r1 - r2)]


def kernel(
    nrow, nphi, rows, cells, tiles, cycles,
    widths_far, hydro, face, diffusion_far, O, F, A,
    H, S, R, SF, RF, FN, Q, M, PX, OM, MG, E,
    widths, diffusion, small_sem, load_sem, send_phi, recv_phi, send_face, recv_face,
    send_mean, recv_mean, send_row, recv_row, pair_ack, far_ack, row_ack,
):
    nvar = hydro.shape[0]
    nface = face.shape[0]
    fields = nvar + nface
    last = tiles - 1
    blocks = cells // SUB
    ring = cells * tiles
    row = lax.axis_index("row")
    phi = lax.axis_index("phi")
    left = lax.rem(phi + nphi - 1, nphi)
    right = lax.rem(phi + 1, nphi)
    pairs = nphi // 2
    pair = phi // 2
    odd = lax.rem(phi, 2)
    partner = phi + 1 - 2 * odd
    far = jnp.where(odd == 1, right, left)
    near_way, far_way = 1 - odd, odd
    packed = 2 * cycles

    loads = [pltpu.make_async_copy(hydro.at[k], H.at[k, pl.ds(2 * ring, rows * ring)], load_sem.at[k]) for k in range(nvar)]
    loads += [pltpu.make_async_copy(face.at[k], F.at[k], load_sem.at[nvar + k]) for k in range(nface)]
    small = [
        pltpu.make_async_copy(widths_far, widths, small_sem.at[0]),
        pltpu.make_async_copy(diffusion_far, diffusion, small_sem.at[1]),
    ]
    for c in small + loads:
        c.start()

    barrier = pltpu.get_barrier_semaphore()

    def greet(**device):
        pl.semaphore_signal(barrier, inc=1, device_id=device, device_id_type=MESH)

    greet(phi=partner)

    @pl.when(far > phi)
    def _():
        greet(phi=far)

    @pl.when(row < nrow - 1)
    def _():
        greet(row=row + 1)

    for step in range(1, pairs):

        @pl.when(pair + step < pairs)
        def _(step=step):
            greet(phi=phi + 2 * step)

    lane = lax.broadcasted_iota(jnp.int32, (1, LANES), 1)
    low = lane < cycles
    high = lane >= LANES - cycles
    mine = [(lane >= packed * f) & (lane < packed * (f + 1)) for f in range(fields)]

    def part(t):
        return slice(t * LANES, (t + 1) * LANES)

    def pack(value, f):
        return pltpu.roll(value, (cycles + packed * f) % LANES, 1)

    def unpack(value, f):
        return pltpu.roll(value, (-(cycles + packed * f)) % LANES, 1)

    def spot(r, b, t):
        start = r * ring + (b * tiles + t) * SUB
        return pl.ds(start if isinstance(r, int) else pl.multiple_of(start, SUB), SUB)

    def layer(r, cell, t):
        return pl.ds(r * ring + (cell // SUB * tiles + t) * SUB + cell % SUB, rows, stride=ring)

    def place(f):
        return (H, f, 2) if f < nvar else (F, f - nvar, 0)

    def halo(way, target, k):
        return pltpu.make_async_remote_copy(
            src_ref=S.at[way, k], dst_ref=R.at[way, k], send_sem=send_phi.at[way, k], recv_sem=recv_phi.at[way, k],
            device_id={"phi": target}, device_id_type=MESH)

    def near_copy(k):
        return halo(near_way, partner, k)

    def far_copy(k):
        return halo(far_way, far, k)

    mean_near = pltpu.make_async_remote_copy(
        src_ref=M, dst_ref=PX, send_sem=send_mean.at[0], recv_sem=recv_mean.at[0],
        device_id={"phi": partner}, device_id_type=MESH)

    def mean_copy(step):
        return pltpu.make_async_remote_copy(
            src_ref=MG.at[pair], dst_ref=MG.at[pair], send_sem=send_mean.at[step], recv_sem=recv_mean.at[step],
            device_id={"phi": lax.rem(phi + 2 * step, nphi)}, device_id_type=MESH)

    def pack_halo(k):
        for t in range(tiles):
            for i in range(2):
                S[0, k, i, t] = H[k, layer(2, i, t), :]
                S[1, k, i, t] = H[k, layer(2, cells - 2 + i, t), :]

    for k in range(nvar):
        loads[k].wait()
        pack_halo(k)
        if k == 0:
            known = 1 + jnp.where(far < phi, 1, 0) + pair + jnp.where(row > 0, 1, 0)
            pl.semaphore_wait(barrier, known)
            for step in range(1, pairs):

                @pl.when(pair >= step)
                def _(step=step):
                    pl.semaphore_signal(pair_ack.at[step], inc=1, device_id={"phi": phi - 2 * step}, device_id_type=MESH)

            @pl.when(far < phi)
            def _():
                pl.semaphore_signal(far_ack, inc=1, device_id={"phi": far}, device_id_type=MESH)

            @pl.when(row > 0)
            def _():
                pl.semaphore_signal(row_ack, inc=1, device_id={"row": row - 1}, device_id_type=MESH)

        if k < EARLY:
            near_copy(k).start()
        if k < MIDDLE:

            @pl.when(phi == nphi - 1)
            def _(k=k):
                far_copy(k).start()

    for c in loads[nvar:]:
        c.wait()
    face_left = pltpu.make_async_remote_copy(
        src_ref=SF, dst_ref=RF, send_sem=send_face, recv_sem=recv_face,
        device_id={"phi": left}, device_id_type=MESH)
    for t in range(tiles):
        SF[t] = F[nface - 1, layer(0, 0, t), :]

    @pl.when(odd == 1)
    def _():
        face_left.start()


    def polar_cells(r, b):
        value = jnp.zeros((SUB, LANES), jnp.float32)
        for f in range(fields):
            ref, k, base = place(f)
            polar = jnp.where(low, ref[k, spot(r + base, b, 0), :], ref[k, spot(r + base, b, last), :])
            value = jnp.where(mine[f], pack(polar, f), value)
        return value

    def cell_mean(r, carry):
        value = jnp.zeros((SUB, LANES), jnp.float32)
        for f in range(fields):
            ref, k, base = place(f)
            sums = [ref[k, spot(r + base, 0, t), :] for t in (0, last)]
            for b in range(1, blocks):
                sums = [x + ref[k, spot(r + base, b, t), :] for x, t in zip(sums, (0, last))]
            value = jnp.where(mine[f], pack(jnp.where(low, sums[0], sums[1]), f), value)
        size = SUB // 2
        while size:
            value = value + pltpu.roll(value, size, 0)
            size //= 2
        M[pl.ds(r, 1), :] = value[0:1] * (1.0 / cells)
        return carry

    lax.fori_loop(0, rows, cell_mean, 0, unroll=4)
    mean_near.start()
    for k in range(EARLY, MIDDLE):
        near_copy(k).start()

    for c in small:
        c.wait()
    width = jnp.zeros((1, LANES), jnp.int32)
    slot = lax.rem(lane, packed)
    for j in range(cycles):
        width = jnp.where(slot == cycles + j, widths[j], width)
        width = jnp.where(slot == j, widths[cycles + j], width)

    index = lax.broadcasted_iota(jnp.int32, (SUB, LANES), 0)

    def local_average(r, carry):
        totals = [polar_cells(r, b) for b in range(blocks)]
        results = list(totals)
        size = 1
        while size < cells:
            if size < SUB:
                turned = []
                for v in totals:
                    forward = pltpu.roll(v, SUB - size, 0)
                    if 2 * size < SUB:
                        forward = jnp.where((index & size) == 0, forward, pltpu.roll(v, size, 0))
                    turned.append(v + forward)
                totals = turned
            else:
                hop = size // SUB
                totals = [totals[b] + totals[b ^ hop] for b in range(blocks)]
            size *= 2
            results = [jnp.where(width == size, v * (1.0 / size), old) for v, old in zip(totals, results)]
        for b in range(blocks):
            Q[pl.ds(pl.multiple_of(r * cells + b * SUB, SUB), SUB), :] = results[b]
        E[0, pl.ds(r, 1), :] = results[0][0:1]
        E[1, pl.ds(r, 1), :] = results[blocks - 1][SUB - 1 : SUB]
        return carry

    lax.fori_loop(0, rows, local_average, 0, unroll=2)

    def put_edges(way, k, i, f, source):
        edges = unpack(E[source], f)
        S[way, k, i, 0] = jnp.where(low, edges, S[way, k, i, 0])
        S[way, k, i, last] = jnp.where(high, edges, S[way, k, i, last])

    for k in range(MIDDLE, nvar):
        for way in range(2):
            put_edges(way, k, 0, k, way)
            if k < 2 * MIDDLE:
                put_edges(way, k, 1, k - MIDDLE, way)
    put_edges(0, nvar - 1, 1, fields - 1, 0)

    for k in range(MIDDLE, nvar):
        near_copy(k).start()

    mean_near.wait_recv()
    MG[pair] = (M[...] + PX[...]) * 0.5
    for step in range(1, pairs):

        @pl.when(pair + step < pairs)
        def _(step=step):
            pl.semaphore_wait(pair_ack.at[step], 1)

        mean_copy(step).start()

    def start_far():
        @pl.when(far > phi)
        def _():
            pl.semaphore_wait(far_ack, 1)

        @pl.when(odd == 0)
        def _():
            edges = unpack(E[0], fields - 1)
            SF[0] = jnp.where(low, edges, SF[0])
            SF[last] = jnp.where(high, edges, SF[last])
            face_left.start()

        @pl.when(phi < nphi - 1)
        def _():
            for k in range(MIDDLE):
                far_copy(k).start()

        for k in range(MIDDLE, nvar):
            far_copy(k).start()

    @pl.when(phi > 0)
    def _():
        start_far()

    for step in range(pairs - 1, 1, -1):
        mean_copy(step).wait_recv()

    @pl.when(phi == 0)
    def _():
        start_far()

    mean_copy(1).wait_recv()

    def group_mean(who):
        result = MG[who // 2]
        size = 2
        while size <= pairs:
            start = (who // (2 * size)) * size
            total = MG[start]
            for i in range(1, size):
                total = total + MG[start + i]
            result = jnp.where(width == 2 * size * cells, total * (1.0 / size), result)
            size *= 2
        return result

    OM[...] = group_mean(phi)
    next_lo = group_mean(right)
    next_hi = group_mean(left)
    wide = width > cells

    def spread(r):
        mean = jnp.broadcast_to(OM[pl.ds(r, 1), :], (SUB, LANES))
        for b in range(blocks):
            where = pl.ds(r * cells + b * SUB if isinstance(r, int) else pl.multiple_of(r * cells + b * SUB, SUB), SUB)
            value = jnp.where(wide, mean, Q[where, :])
            for f in range(fields):
                ref, k, base = place(f)
                polar = unpack(value, f)
                ref[k, spot(r + base, b, 0), :] = jnp.where(low, polar, ref[k, spot(r + base, b, 0), :])
                ref[k, spot(r + base, b, last), :] = jnp.where(high, polar, ref[k, spot(r + base, b, last), :])

    for r in (0, 1, rows - 2, rows - 1):
        spread(r)

    down = pltpu.make_async_remote_copy(
        src_ref=H.at[:, pl.ds(2 * ring, 2 * ring)], dst_ref=H.at[:, pl.ds((rows + 2) * ring, 2 * ring)],
        send_sem=send_row.at[0], recv_sem=recv_row.at[0], device_id={"row": row - 1}, device_id_type=MESH)
    down_face = pltpu.make_async_remote_copy(
        src_ref=F.at[0, pl.ds(0, ring)], dst_ref=FN,
        send_sem=send_row.at[1], recv_sem=recv_row.at[1], device_id={"row": row - 1}, device_id_type=MESH)
    up = pltpu.make_async_remote_copy(
        src_ref=H.at[:, pl.ds(rows * ring, 2 * ring)], dst_ref=H.at[:, pl.ds(0, 2 * ring)],
        send_sem=send_row.at[2], recv_sem=recv_row.at[2], device_id={"row": row + 1}, device_id_type=MESH)

    @pl.when(row > 0)
    def _():
        down.start()
        down_face.start()

    @pl.when(row < nrow - 1)
    def _():
        pl.semaphore_wait(row_ack, 1)
        up.start()

    lax.fori_loop(2, rows - 2, lambda r, c: (spread(r), c)[1], 0, unroll=4)

    @pl.when(row == 0)
    def _():
        H[:, pl.ds(0, 2 * ring), :] = jnp.zeros((nvar, 2 * ring, LANES), jnp.float32)

    @pl.when(row == nrow - 1)
    def _():
        H[:, pl.ds((rows + 2) * ring, 2 * ring), :] = jnp.zeros((nvar, 2 * ring, LANES), jnp.float32)
        FN[...] = jnp.zeros_like(FN)

    def whole(ref, k, r, t):
        return jnp.concatenate([ref[k, spot(r, b, t), :] for b in range(blocks)], 0)

    def write(k, r, t, value):
        for b in range(blocks):
            O[k, spot(r, b, t), :] = value[b * SUB : (b + 1) * SUB]

    def shifted(parts, amount):
        out = []
        turned = [pltpu.roll(p, (-amount) % LANES, 1) for p in parts]
        for t in range(tiles):
            if amount > 0:
                inside = lane < LANES - amount
                other = turned[t + 1] if t + 1 < tiles else 0.0
            else:
                inside = lane >= -amount
                other = turned[t - 1] if t > 0 else 0.0
            out.append(jnp.where(inside, turned[t], other))
        return out

    def smooth_row(r):
        for k in range(nvar):
            mid = [whole(H, k, r + 2, t) for t in range(tiles)]
            one = [a + b for a, b in zip(shifted(mid, 1), shifted(mid, -1))]
            two = [a + b for a, b in zip(shifted(mid, 2), shifted(mid, -2))]
            for t in range(tiles):
                v = mid[t]
                s1 = one[t] + (pltpu.roll(v, 1, 0) + pltpu.roll(v, cells - 1, 0)) + (whole(H, k, r + 1, t) + whole(H, k, r + 3, t))
                s2 = two[t] + (pltpu.roll(v, 2, 0) + pltpu.roll(v, cells - 2, 0)) + (whole(H, k, r, t) + whole(H, k, r + 4, t))
                change = (16.0 * s1 - s2 - 90.0 * v) * (1.0 / 12.0)
                write(k, r, t, v + diffusion[k : k + 1, part(t)] * change)

    def field_row(r, following):
        polar = [whole(F, 1, r, t) for t in range(tiles)]
        polar_next = shifted(polar, 1)
        for t in range(tiles):
            write(nvar, r, t, 0.5 * (whole(F, 0, r, t) + following(t)))
            write(nvar + 1, r, t, 0.5 * (polar[t] + polar_next[t]))
            azimuth = whole(F, 2, r, t)
            write(nvar + 2, r, t, 0.5 * (azimuth + pltpu.roll(azimuth, cells - 1, 0)))

    def inner_row(r, carry):
        field_row(r, lambda t: whole(F, 0, r + 1, t))
        smooth_row(r)
        return carry

    lax.fori_loop(2, rows - 2, inner_row, 0, unroll=2)
    for r in (0, 1, rows - 2):
        field_row(r, lambda t, r=r: whole(F, 0, r + 1, t))

    @pl.when(row > 0)
    def _():
        up.wait_recv()

    @pl.when(row < nrow - 1)
    def _():
        down.wait_recv()
        down_face.wait_recv()

    field_row(rows - 1, lambda t: jnp.concatenate([FN[spot(0, b, t), :] for b in range(blocks)], 0))
    for r in (0, 1, rows - 2, rows - 1):
        smooth_row(r)

    local = unpack(width, 0) <= cells
    ends = (0, 1, cells - 2, cells - 1)

    def sent_edge(way, k, t):
        return R[way, k, 0, t] if k >= MIDDLE else R[way, k + MIDDLE, 1, t]

    def patch(k):
        mean_l = unpack(next_hi, k)
        mean_r = unpack(next_lo, k)
        for t in range(tiles):
            edge_l = jnp.where(local, sent_edge(1, k, t), mean_l)
            edge_r = jnp.where(local, sent_edge(0, k, t), mean_r)
            terms = halo_terms(
                diffusion[k : k + 1, part(t)] * (1.0 / 12.0),
                [fix_polar(low, high, last, R[1, k, i, t], edge_l, t) for i in range(2)],
                [fix_polar(low, high, last, R[0, k, i, t], edge_r, t) for i in range(2)],
                [H[k, layer(2, cell, t), :] for cell in ends])
            for cell, term in zip(ends, terms):
                O[k, layer(0, cell, t), :] = O[k, layer(0, cell, t), :] + term

    def arrive(k):
        halo(1, right, k).wait_recv()
        halo(0, left, k).wait_recv()

    slots, _ = late_slots(tiles)
    final = nvar - 1
    A[slots["mean_left"]] = unpack(next_hi, final)
    A[slots["mean_right"]] = unpack(next_lo, final)
    A[slots["mean_face"]] = unpack(next_lo, fields - 1)
    A[slots["local"]] = jnp.broadcast_to(jnp.where(local, 1.0, 0.0), (rows, LANES))
    for t in range(tiles):
        A[slots["scale"] + t] = jnp.broadcast_to(diffusion[final : final + 1, part(t)] * (1.0 / 12.0), (rows, LANES))
        for i, cell in enumerate(ends):
            A[slots["inner"] + 4 * t + i] = H[final, layer(2, cell, t), :]
    for k in range(MIDDLE):
        arrive(k)
    face_left.wait_recv()
    for t in range(tiles):
        A[slots["face"] + t] = RF[t]
    for k in range(MIDDLE, final):
        arrive(k)
        if k < 2 * MIDDLE:
            patch(k - MIDDLE)
        patch(k)
    arrive(final)
    for t in range(tiles):
        A[slots["face_edge"] + t] = jnp.where(odd == 0, R[0, final, 1, t], RF[t])
        for way in range(2):
            for i in range(2):
                A[slots["halo"] + 4 * t + 2 * way + i] = R[way, final, i, t]

    for k in range(nvar):
        near_copy(k).wait_send()
        far_copy(k).wait_send()
    face_left.wait_send()
    mean_near.wait_send()
    for step in range(1, pairs):
        mean_copy(step).wait_send()

    @pl.when(row > 0)
    def _():
        down.wait_send()
        down_face.wait_send()

    @pl.when(row < nrow - 1)
    def _():
        up.wait_send()


def spill(nvar, rows, cells, tiles, cycles, conserved, faces, A, conserved_out, faces_out, P, sem):
    fields = conserved.shape[0]
    nface = faces.shape[0]
    ring = cells * tiles
    last = tiles - 1
    late = (nvar - 1, fields - 1)

    def layer(cell, t):
        return pl.ds((cell // SUB * tiles + t) * SUB + cell % SUB, rows, stride=ring)

    def out(k, source):
        return pltpu.make_async_copy(source, conserved_out.at[k], sem.at[k])

    copies = [out(k, conserved.at[k]) for k in range(fields) if k not in late]
    copies += [pltpu.make_async_copy(faces.at[k], faces_out.at[k], sem.at[fields + k]) for k in range(nface)]
    for c in copies:
        c.start()

    slots, _ = late_slots(tiles)
    lane = lax.broadcasted_iota(jnp.int32, (1, LANES), 1)
    low = lane < cycles
    high = lane >= LANES - cycles
    local = A[slots["local"]] > 0.5
    ends = (0, 1, cells - 2, cells - 1)
    for n, k in enumerate(late):
        P[n] = conserved[k]
    for t in range(tiles):
        halo = [A[slots["halo"] + 4 * t + i] for i in range(4)]
        edge_l = jnp.where(local, halo[2], A[slots["mean_left"]])
        edge_r = jnp.where(local, halo[0], A[slots["mean_right"]])
        terms = halo_terms(
            A[slots["scale"] + t],
            [fix_polar(low, high, last, v, edge_l, t) for v in halo[2:]],
            [fix_polar(low, high, last, v, edge_r, t) for v in halo[:2]],
            [A[slots["inner"] + 4 * t + i] for i in range(4)])
        for cell, term in zip(ends, terms):
            P[0, layer(cell, t), :] = P[0, layer(cell, t), :] + term
    copies.append(out(late[0], P.at[0]))
    copies[-1].start()
    for t in range(tiles):
        edge = jnp.where(local, A[slots["face_edge"] + t], A[slots["mean_face"]])
        following = fix_polar(low, high, last, A[slots["face"] + t], edge, t)
        P[1, layer(cells - 1, t), :] = 0.5 * (faces[nface - 1, layer(cells - 1, t), :] + following)
    copies.append(out(late[1], P.at[1]))
    copies[-1].start()
    for c in copies:
        c.wait()


def blocked(x):
    n, rows, cells, theta = x.shape
    x = x.reshape(n, rows, cells // SUB, SUB, theta // LANES, LANES)
    return x.transpose(0, 1, 2, 4, 3, 5).reshape(n, rows * cells * (theta // LANES), LANES)


def unblocked(x, rows, cells, theta):
    x = x.reshape(x.shape[0], rows, cells // SUB, theta // LANES, SUB, LANES)
    return x.transpose(0, 1, 2, 4, 3, 5).reshape(x.shape[0], rows, cells, theta)


def body(nrow, nphi, hydro_vars, face_b, widths, diffusion):
    nvar, rows, cells, theta = hydro_vars.shape
    nface = face_b.shape[0]
    fields = nvar + nface
    cycles = widths.shape[0] // 2
    tiles = theta // LANES
    ring = cells * tiles
    f32 = jnp.float32
    shape = lambda *s: pltpu.VMEM(s, f32)
    far = pl.BlockSpec(memory_space=pltpu.HBM)
    near = pl.BlockSpec(memory_space=pltpu.VMEM)
    result_bytes = ((fields + nface) * ring + late_slots(tiles)[1]) * rows * LANES * 4
    slots = late_slots(tiles)[1]
    conserved, faces, late = pl.pallas_call(
        functools.partial(kernel, nrow, nphi, rows, cells, tiles, cycles),
        out_shape=(
            pltpu.VMEM((fields, rows * ring, LANES), f32),
            pltpu.VMEM((nface, rows * ring, LANES), f32),
            pltpu.VMEM((slots, rows, LANES), f32),
        ),
        in_specs=[far, far, far, far],
        out_specs=(near, near, near),
        scratch_shapes=[
            shape(nvar, (rows + 4) * ring, LANES),
            shape(2, nvar, 2, tiles, rows, LANES),
            shape(2, nvar, 2, tiles, rows, LANES),
            shape(tiles, rows, LANES),
            shape(tiles, rows, LANES),
            shape(ring, LANES),
            shape(rows * cells, LANES),
            shape(rows, LANES),
            shape(rows, LANES),
            shape(rows, LANES),
            shape(nphi // 2, rows, LANES),
            shape(2, rows, LANES),
            pltpu.SMEM((2 * cycles,), jnp.int32),
            shape(nvar, theta),
            pltpu.SemaphoreType.DMA((2,)),
            pltpu.SemaphoreType.DMA((fields,)),
            pltpu.SemaphoreType.DMA((2, nvar)),
            pltpu.SemaphoreType.DMA((2, nvar)),
            pltpu.SemaphoreType.DMA,
            pltpu.SemaphoreType.DMA,
            pltpu.SemaphoreType.DMA((nphi // 2,)),
            pltpu.SemaphoreType.DMA((nphi // 2,)),
            pltpu.SemaphoreType.DMA((3,)),
            pltpu.SemaphoreType.DMA((3,)),
            pltpu.SemaphoreType.REGULAR((nphi // 2,)),
            pltpu.SemaphoreType.REGULAR,
            pltpu.SemaphoreType.REGULAR,
        ],
        compiler_params=pltpu.CompilerParams(
            collective_id=0, has_side_effects=True, vmem_limit_bytes=LIMIT - result_bytes
        ),
        name="step",
    )(widths, blocked(hydro_vars), blocked(face_b), diffusion)
    conserved, faces = pl.pallas_call(
        functools.partial(spill, nvar, rows, cells, tiles, cycles),
        out_shape=(
            jax.ShapeDtypeStruct((fields, rows * ring, LANES), f32),
            jax.ShapeDtypeStruct((nface, rows * ring, LANES), f32),
        ),
        in_specs=[near, near, near],
        out_specs=(far, far),
        scratch_shapes=[shape(2, rows * ring, LANES), pltpu.SemaphoreType.DMA((fields + nface,))],
        compiler_params=pltpu.CompilerParams(vmem_limit_bytes=8 * rows * ring * LANES + 2000000),
        name="spill",
    )(conserved, faces, late)
    return unblocked(conserved, rows, cells, theta), unblocked(faces, rows, cells, theta)


def solution(mesh):
    spec = P(None, "row", "phi", None)
    return jax.shard_map(
        functools.partial(body, mesh.shape["row"], mesh.shape["phi"]),
        mesh=mesh,
        in_specs=(spec, spec, P(), P()),
        out_specs=(spec, spec),
        check_vma=False,
    )
```

```python
import functools

import jax
import jax.numpy as jnp
from jax import lax
from jax.experimental import pallas as pl
from jax.experimental.pallas import tpu as pltpu
from jax.sharding import PartitionSpec as P

MESH = pl.DeviceIdType.MESH
LANES = 128
SUB = 8
EARLY = 1
MIDDLE = 2
HELD_NEAR = 2
HELD_FAR = 2
LIMIT = 58000000


def late_slots(tiles):
    names = ["halo", "inner", "face", "face_edge", "scale"]
    sizes = [4 * tiles, 4 * tiles, tiles, tiles, tiles]
    starts, total = {}, 0
    for name, size in zip(names, sizes):
        starts[name] = total
        total += size
    for name in ("mean_left", "mean_right", "mean_face", "local"):
        starts[name] = total
        total += 1
    return starts, total


def fix_polar(low, high, last, raw, edge, t):
    if t == 0:
        raw = jnp.where(low, edge, raw)
    if t == last:
        raw = jnp.where(high, edge, raw)
    return raw


def halo_terms(scale, from_left, from_right, inner):
    l1, l2 = from_left[1] - inner[3], from_left[0] - inner[2]
    r1, r2 = from_right[0] - inner[0], from_right[1] - inner[1]
    return [scale * term for term in (16.0 * l1 - l2, -l1, -r1, 16.0 * r1 - r2)]


def kernel(
    nrow, nphi, rows, cells, tiles, cycles,
    widths_far, hydro, face, diffusion_far, O, F, A,
    H, S, R, SF, RF, FN, Q, M, PX, OM, MG, E,
    widths, diffusion, small_sem, load_sem, send_phi, recv_phi, send_face, recv_face,
    send_mean, recv_mean, send_row, recv_row, pair_ack, far_ack, row_ack,
):
    nvar = hydro.shape[0]
    nface = face.shape[0]
    fields = nvar + nface
    last = tiles - 1
    blocks = cells // SUB
    ring = cells * tiles
    row = lax.axis_index("row")
    phi = lax.axis_index("phi")
    left = lax.rem(phi + nphi - 1, nphi)
    right = lax.rem(phi + 1, nphi)
    pairs = nphi // 2
    pair = phi // 2
    odd = lax.rem(phi, 2)
    partner = phi + 1 - 2 * odd
    far = jnp.where(odd == 1, right, left)
    near_way, far_way = 1 - odd, odd
    yields_near = (phi == 1) & (lax.rem(row, 2) == 1)
    yields_far = (phi == nphi - 1) & (lax.rem(row, 2) == 1)
    packed = 2 * cycles

    loads = [pltpu.make_async_copy(hydro.at[k], H.at[k, pl.ds(2 * ring, rows * ring)], load_sem.at[k]) for k in range(nvar)]
    loads += [pltpu.make_async_copy(face.at[k], F.at[k], load_sem.at[nvar + k]) for k in range(nface)]
    small = [
        pltpu.make_async_copy(widths_far, widths, small_sem.at[0]),
        pltpu.make_async_copy(diffusion_far, diffusion, small_sem.at[1]),
    ]
    for c in small + loads:
        c.start()

    barrier = pltpu.get_barrier_semaphore()

    def greet(**device):
        pl.semaphore_signal(barrier, inc=1, device_id=device, device_id_type=MESH)

    greet(phi=partner)

    @pl.when(far > phi)
    def _():
        greet(phi=far)

    @pl.when(row < nrow - 1)
    def _():
        greet(row=row + 1)

    for step in range(1, pairs):

        @pl.when(pair + step < pairs)
        def _(step=step):
            greet(phi=phi + 2 * step)

    lane = lax.broadcasted_iota(jnp.int32, (1, LANES), 1)
    low = lane < cycles
    high = lane >= LANES - cycles
    mine = [(lane >= packed * f) & (lane < packed * (f + 1)) for f in range(fields)]

    def part(t):
        return slice(t * LANES, (t + 1) * LANES)

    def pack(value, f):
        return pltpu.roll(value, (cycles + packed * f) % LANES, 1)

    def unpack(value, f):
        return pltpu.roll(value, (-(cycles + packed * f)) % LANES, 1)

    def spot(r, b, t):
        start = r * ring + (b * tiles + t) * SUB
        return pl.ds(start if isinstance(r, int) else pl.multiple_of(start, SUB), SUB)

    def layer(r, cell, t):
        return pl.ds(r * ring + (cell // SUB * tiles + t) * SUB + cell % SUB, rows, stride=ring)

    def place(f):
        return (H, f, 2) if f < nvar else (F, f - nvar, 0)

    def halo(way, target, k):
        return pltpu.make_async_remote_copy(
            src_ref=S.at[way, k], dst_ref=R.at[way, k], send_sem=send_phi.at[way, k], recv_sem=recv_phi.at[way, k],
            device_id={"phi": target}, device_id_type=MESH)

    def near_copy(k):
        return halo(near_way, partner, k)

    def far_copy(k):
        return halo(far_way, far, k)

    mean_near = pltpu.make_async_remote_copy(
        src_ref=M, dst_ref=PX, send_sem=send_mean.at[0], recv_sem=recv_mean.at[0],
        device_id={"phi": partner}, device_id_type=MESH)

    def mean_copy(step):
        return pltpu.make_async_remote_copy(
            src_ref=MG.at[pair], dst_ref=MG.at[pair], send_sem=send_mean.at[step], recv_sem=recv_mean.at[step],
            device_id={"phi": lax.rem(phi + 2 * step, nphi)}, device_id_type=MESH)

    def pack_halo(k):
        for t in range(tiles):
            for i in range(2):
                S[0, k, i, t] = H[k, layer(2, i, t), :]
                S[1, k, i, t] = H[k, layer(2, cells - 2 + i, t), :]

    for k in range(nvar):
        loads[k].wait()
        pack_halo(k)
        if k == 0:
            known = 1 + jnp.where(far < phi, 1, 0) + pair + jnp.where(row > 0, 1, 0)
            pl.semaphore_wait(barrier, known)
            for step in range(1, pairs):

                @pl.when(pair >= step)
                def _(step=step):
                    pl.semaphore_signal(pair_ack.at[step], inc=1, device_id={"phi": phi - 2 * step}, device_id_type=MESH)

            @pl.when(far < phi)
            def _():
                pl.semaphore_signal(far_ack, inc=1, device_id={"phi": far}, device_id_type=MESH)

            @pl.when(row > 0)
            def _():
                pl.semaphore_signal(row_ack, inc=1, device_id={"row": row - 1}, device_id_type=MESH)

        if k < EARLY:
            near_copy(k).start()
        if k < MIDDLE:

            @pl.when(phi == nphi - 1)
            def _(k=k):
                far_copy(k).start()

    for c in loads[nvar:]:
        c.wait()
    face_left = pltpu.make_async_remote_copy(
        src_ref=SF, dst_ref=RF, send_sem=send_face, recv_sem=recv_face,
        device_id={"phi": left}, device_id_type=MESH)
    for t in range(tiles):
        SF[t] = F[nface - 1, layer(0, 0, t), :]

    @pl.when(odd == 1)
    def _():
        face_left.start()


    def polar_cells(r, b):
        value = jnp.zeros((SUB, LANES), jnp.float32)
        for f in range(fields):
            ref, k, base = place(f)
            polar = jnp.where(low, ref[k, spot(r + base, b, 0), :], ref[k, spot(r + base, b, last), :])
            value = jnp.where(mine[f], pack(polar, f), value)
        return value

    def cell_mean(r, carry):
        value = jnp.zeros((SUB, LANES), jnp.float32)
        for f in range(fields):
            ref, k, base = place(f)
            sums = [ref[k, spot(r + base, 0, t), :] for t in (0, last)]
            for b in range(1, blocks):
                sums = [x + ref[k, spot(r + base, b, t), :] for x, t in zip(sums, (0, last))]
            value = jnp.where(mine[f], pack(jnp.where(low, sums[0], sums[1]), f), value)
        size = SUB // 2
        while size:
            value = value + pltpu.roll(value, size, 0)
            size //= 2
        M[pl.ds(r, 1), :] = value[0:1] * (1.0 / cells)
        return carry

    lax.fori_loop(0, rows, cell_mean, 0, unroll=4)
    mean_near.start()
    for k in range(EARLY, MIDDLE):
        near_copy(k).start()

    for c in small:
        c.wait()
    width = jnp.zeros((1, LANES), jnp.int32)
    slot = lax.rem(lane, packed)
    for j in range(cycles):
        width = jnp.where(slot == cycles + j, widths[j], width)
        width = jnp.where(slot == j, widths[cycles + j], width)

    index = lax.broadcasted_iota(jnp.int32, (SUB, LANES), 0)

    def local_average(r, carry):
        totals = [polar_cells(r, b) for b in range(blocks)]
        results = list(totals)
        size = 1
        while size < cells:
            if size < SUB:
                turned = []
                for v in totals:
                    forward = pltpu.roll(v, SUB - size, 0)
                    if 2 * size < SUB:
                        forward = jnp.where((index & size) == 0, forward, pltpu.roll(v, size, 0))
                    turned.append(v + forward)
                totals = turned
            else:
                hop = size // SUB
                totals = [totals[b] + totals[b ^ hop] for b in range(blocks)]
            size *= 2
            results = [jnp.where(width == size, v * (1.0 / size), old) for v, old in zip(totals, results)]
        for b in range(blocks):
            Q[pl.ds(pl.multiple_of(r * cells + b * SUB, SUB), SUB), :] = results[b]
        E[0, pl.ds(r, 1), :] = results[0][0:1]
        E[1, pl.ds(r, 1), :] = results[blocks - 1][SUB - 1 : SUB]
        return carry

    lax.fori_loop(0, rows, local_average, 0, unroll=2)

    def put_edges(way, k, i, f, source):
        edges = unpack(E[source], f)
        S[way, k, i, 0] = jnp.where(low, edges, S[way, k, i, 0])
        S[way, k, i, last] = jnp.where(high, edges, S[way, k, i, last])

    for k in range(MIDDLE, nvar):
        for way in range(2):
            put_edges(way, k, 0, k, way)
            if k < 2 * MIDDLE:
                put_edges(way, k, 1, k - MIDDLE, way)
    put_edges(0, nvar - 1, 1, fields - 1, 0)

    for k in range(MIDDLE, HELD_NEAR):
        near_copy(k).start()

    @pl.when(jnp.logical_not(yields_near))
    def _():
        for k in range(HELD_NEAR, nvar):
            near_copy(k).start()


    mean_near.wait_recv()
    MG[pair] = (M[...] + PX[...]) * 0.5
    for step in range(1, pairs):

        @pl.when(pair + step < pairs)
        def _(step=step):
            pl.semaphore_wait(pair_ack.at[step], 1)

        mean_copy(step).start()

    def start_far():
        @pl.when(far > phi)
        def _():
            pl.semaphore_wait(far_ack, 1)

        @pl.when(odd == 0)
        def _():
            edges = unpack(E[0], fields - 1)
            SF[0] = jnp.where(low, edges, SF[0])
            SF[last] = jnp.where(high, edges, SF[last])
            face_left.start()

        @pl.when(phi < nphi - 1)
        def _():
            for k in range(MIDDLE):
                far_copy(k).start()

        for k in range(MIDDLE, HELD_FAR):
            far_copy(k).start()

        @pl.when(jnp.logical_not(yields_far))
        def _():
            for k in range(HELD_FAR, nvar):
                far_copy(k).start()

    @pl.when(phi > 0)
    def _():
        start_far()

    for step in range(pairs - 1, 1, -1):
        mean_copy(step).wait_recv()

    @pl.when(phi == 0)
    def _():
        start_far()

    mean_copy(1).wait_recv()

    def group_mean(who):
        result = MG[who // 2]
        size = 2
        while size <= pairs:
            start = (who // (2 * size)) * size
            total = MG[start]
            for i in range(1, size):
                total = total + MG[start + i]
            result = jnp.where(width == 2 * size * cells, total * (1.0 / size), result)
            size *= 2
        return result

    OM[...] = group_mean(phi)
    next_lo = group_mean(right)
    next_hi = group_mean(left)
    wide = width > cells

    def spread(r):
        mean = jnp.broadcast_to(OM[pl.ds(r, 1), :], (SUB, LANES))
        for b in range(blocks):
            where = pl.ds(r * cells + b * SUB if isinstance(r, int) else pl.multiple_of(r * cells + b * SUB, SUB), SUB)
            value = jnp.where(wide, mean, Q[where, :])
            for f in range(fields):
                ref, k, base = place(f)
                polar = unpack(value, f)
                ref[k, spot(r + base, b, 0), :] = jnp.where(low, polar, ref[k, spot(r + base, b, 0), :])
                ref[k, spot(r + base, b, last), :] = jnp.where(high, polar, ref[k, spot(r + base, b, last), :])

    for r in (0, 1, rows - 2, rows - 1):
        spread(r)

    down = pltpu.make_async_remote_copy(
        src_ref=H.at[:, pl.ds(2 * ring, 2 * ring)], dst_ref=H.at[:, pl.ds((rows + 2) * ring, 2 * ring)],
        send_sem=send_row.at[0], recv_sem=recv_row.at[0], device_id={"row": row - 1}, device_id_type=MESH)
    down_face = pltpu.make_async_remote_copy(
        src_ref=F.at[0, pl.ds(0, ring)], dst_ref=FN,
        send_sem=send_row.at[1], recv_sem=recv_row.at[1], device_id={"row": row - 1}, device_id_type=MESH)
    up = pltpu.make_async_remote_copy(
        src_ref=H.at[:, pl.ds(rows * ring, 2 * ring)], dst_ref=H.at[:, pl.ds(0, 2 * ring)],
        send_sem=send_row.at[2], recv_sem=recv_row.at[2], device_id={"row": row + 1}, device_id_type=MESH)

    @pl.when(row > 0)
    def _():
        down.start()
        down_face.start()

    @pl.when(row < nrow - 1)
    def _():
        pl.semaphore_wait(row_ack, 1)
        up.start()

    lax.fori_loop(2, rows - 2, lambda r, c: (spread(r), c)[1], 0, unroll=4)

    @pl.when(yields_near)
    def _():
        for k in range(HELD_NEAR, nvar):
            near_copy(k).start()

    @pl.when(yields_far)
    def _():
        for k in range(HELD_FAR, nvar):
            far_copy(k).start()

    @pl.when(row == 0)
    def _():
        H[:, pl.ds(0, 2 * ring), :] = jnp.zeros((nvar, 2 * ring, LANES), jnp.float32)

    @pl.when(row == nrow - 1)
    def _():
        H[:, pl.ds((rows + 2) * ring, 2 * ring), :] = jnp.zeros((nvar, 2 * ring, LANES), jnp.float32)
        FN[...] = jnp.zeros_like(FN)

    def whole(ref, k, r, t):
        return jnp.concatenate([ref[k, spot(r, b, t), :] for b in range(blocks)], 0)

    def write(k, r, t, value):
        for b in range(blocks):
            O[k, spot(r, b, t), :] = value[b * SUB : (b + 1) * SUB]

    def shifted(parts, amount):
        out = []
        turned = [pltpu.roll(p, (-amount) % LANES, 1) for p in parts]
        for t in range(tiles):
            if amount > 0:
                inside = lane < LANES - amount
                other = turned[t + 1] if t + 1 < tiles else 0.0
            else:
                inside = lane >= -amount
                other = turned[t - 1] if t > 0 else 0.0
            out.append(jnp.where(inside, turned[t], other))
        return out

    def smooth_row(r):
        for k in range(nvar):
            mid = [whole(H, k, r + 2, t) for t in range(tiles)]
            one = [a + b for a, b in zip(shifted(mid, 1), shifted(mid, -1))]
            two = [a + b for a, b in zip(shifted(mid, 2), shifted(mid, -2))]
            for t in range(tiles):
                v = mid[t]
                s1 = one[t] + (pltpu.roll(v, 1, 0) + pltpu.roll(v, cells - 1, 0)) + (whole(H, k, r + 1, t) + whole(H, k, r + 3, t))
                s2 = two[t] + (pltpu.roll(v, 2, 0) + pltpu.roll(v, cells - 2, 0)) + (whole(H, k, r, t) + whole(H, k, r + 4, t))
                change = (16.0 * s1 - s2 - 90.0 * v) * (1.0 / 12.0)
                write(k, r, t, v + diffusion[k : k + 1, part(t)] * change)

    def field_row(r, following):
        polar = [whole(F, 1, r, t) for t in range(tiles)]
        polar_next = shifted(polar, 1)
        for t in range(tiles):
            write(nvar, r, t, 0.5 * (whole(F, 0, r, t) + following(t)))
            write(nvar + 1, r, t, 0.5 * (polar[t] + polar_next[t]))
            azimuth = whole(F, 2, r, t)
            write(nvar + 2, r, t, 0.5 * (azimuth + pltpu.roll(azimuth, cells - 1, 0)))

    def inner_row(r, carry):
        field_row(r, lambda t: whole(F, 0, r + 1, t))
        smooth_row(r)
        return carry

    lax.fori_loop(2, rows - 2, inner_row, 0, unroll=4)
    for r in (0, 1, rows - 2):
        field_row(r, lambda t, r=r: whole(F, 0, r + 1, t))

    @pl.when(row > 0)
    def _():
        up.wait_recv()

    @pl.when(row < nrow - 1)
    def _():
        down.wait_recv()
        down_face.wait_recv()

    field_row(rows - 1, lambda t: jnp.concatenate([FN[spot(0, b, t), :] for b in range(blocks)], 0))
    for r in (0, 1, rows - 2, rows - 1):
        smooth_row(r)

    local = unpack(width, 0) <= cells
    ends = (0, 1, cells - 2, cells - 1)

    def sent_edge(way, k, t):
        return R[way, k, 0, t] if k >= MIDDLE else R[way, k + MIDDLE, 1, t]

    def patch(k):
        mean_l = unpack(next_hi, k)
        mean_r = unpack(next_lo, k)
        for t in range(tiles):
            edge_l = jnp.where(local, sent_edge(1, k, t), mean_l)
            edge_r = jnp.where(local, sent_edge(0, k, t), mean_r)
            terms = halo_terms(
                diffusion[k : k + 1, part(t)] * (1.0 / 12.0),
                [fix_polar(low, high, last, R[1, k, i, t], edge_l, t) for i in range(2)],
                [fix_polar(low, high, last, R[0, k, i, t], edge_r, t) for i in range(2)],
                [H[k, layer(2, cell, t), :] for cell in ends])
            for cell, term in zip(ends, terms):
                O[k, layer(0, cell, t), :] = O[k, layer(0, cell, t), :] + term

    def arrive(k):
        halo(1, right, k).wait_recv()
        halo(0, left, k).wait_recv()

    slots, _ = late_slots(tiles)
    final = nvar - 1
    A[slots["mean_left"]] = unpack(next_hi, final)
    A[slots["mean_right"]] = unpack(next_lo, final)
    A[slots["mean_face"]] = unpack(next_lo, fields - 1)
    A[slots["local"]] = jnp.broadcast_to(jnp.where(local, 1.0, 0.0), (rows, LANES))
    for t in range(tiles):
        A[slots["scale"] + t] = jnp.broadcast_to(diffusion[final : final + 1, part(t)] * (1.0 / 12.0), (rows, LANES))
        for i, cell in enumerate(ends):
            A[slots["inner"] + 4 * t + i] = H[final, layer(2, cell, t), :]
    for k in range(MIDDLE):
        arrive(k)
    face_left.wait_recv()
    for t in range(tiles):
        A[slots["face"] + t] = RF[t]
    for k in range(MIDDLE, final):
        arrive(k)
        if k < 2 * MIDDLE:
            patch(k - MIDDLE)
        patch(k)
    arrive(final)
    for t in range(tiles):
        A[slots["face_edge"] + t] = jnp.where(odd == 0, R[0, final, 1, t], RF[t])
        for way in range(2):
            for i in range(2):
                A[slots["halo"] + 4 * t + 2 * way + i] = R[way, final, i, t]

    for k in range(nvar):
        near_copy(k).wait_send()
        far_copy(k).wait_send()
    face_left.wait_send()
    mean_near.wait_send()
    for step in range(1, pairs):
        mean_copy(step).wait_send()

    @pl.when(row > 0)
    def _():
        down.wait_send()
        down_face.wait_send()

    @pl.when(row < nrow - 1)
    def _():
        up.wait_send()


def spill(nvar, rows, cells, tiles, cycles, conserved, faces, A, conserved_out, faces_out, P, sem):
    fields = conserved.shape[0]
    nface = faces.shape[0]
    ring = cells * tiles
    last = tiles - 1
    late = (nvar - 1, fields - 1)

    def layer(cell, t):
        return pl.ds((cell // SUB * tiles + t) * SUB + cell % SUB, rows, stride=ring)

    def out(k, source):
        return pltpu.make_async_copy(source, conserved_out.at[k], sem.at[k])

    copies = [out(k, conserved.at[k]) for k in range(fields) if k not in late]
    copies += [pltpu.make_async_copy(faces.at[k], faces_out.at[k], sem.at[fields + k]) for k in range(nface)]
    for c in copies:
        c.start()

    slots, _ = late_slots(tiles)
    lane = lax.broadcasted_iota(jnp.int32, (1, LANES), 1)
    low = lane < cycles
    high = lane >= LANES - cycles
    local = A[slots["local"]] > 0.5
    ends = (0, 1, cells - 2, cells - 1)
    for n, k in enumerate(late):
        P[n] = conserved[k]
    for t in range(tiles):
        halo = [A[slots["halo"] + 4 * t + i] for i in range(4)]
        edge_l = jnp.where(local, halo[2], A[slots["mean_left"]])
        edge_r = jnp.where(local, halo[0], A[slots["mean_right"]])
        terms = halo_terms(
            A[slots["scale"] + t],
            [fix_polar(low, high, last, v, edge_l, t) for v in halo[2:]],
            [fix_polar(low, high, last, v, edge_r, t) for v in halo[:2]],
            [A[slots["inner"] + 4 * t + i] for i in range(4)])
        for cell, term in zip(ends, terms):
            P[0, layer(cell, t), :] = P[0, layer(cell, t), :] + term
    copies.append(out(late[0], P.at[0]))
    copies[-1].start()
    for t in range(tiles):
        edge = jnp.where(local, A[slots["face_edge"] + t], A[slots["mean_face"]])
        following = fix_polar(low, high, last, A[slots["face"] + t], edge, t)
        P[1, layer(cells - 1, t), :] = 0.5 * (faces[nface - 1, layer(cells - 1, t), :] + following)
    copies.append(out(late[1], P.at[1]))
    copies[-1].start()
    for c in copies:
        c.wait()


def blocked(x):
    n, rows, cells, theta = x.shape
    x = x.reshape(n, rows, cells // SUB, SUB, theta // LANES, LANES)
    return x.transpose(0, 1, 2, 4, 3, 5).reshape(n, rows * cells * (theta // LANES), LANES)


def unblocked(x, rows, cells, theta):
    x = x.reshape(x.shape[0], rows, cells // SUB, theta // LANES, SUB, LANES)
    return x.transpose(0, 1, 2, 4, 3, 5).reshape(x.shape[0], rows, cells, theta)


def body(nrow, nphi, hydro_vars, face_b, widths, diffusion):
    nvar, rows, cells, theta = hydro_vars.shape
    nface = face_b.shape[0]
    fields = nvar + nface
    cycles = widths.shape[0] // 2
    tiles = theta // LANES
    ring = cells * tiles
    f32 = jnp.float32
    shape = lambda *s: pltpu.VMEM(s, f32)
    far = pl.BlockSpec(memory_space=pltpu.HBM)
    near = pl.BlockSpec(memory_space=pltpu.VMEM)
    result_bytes = ((fields + nface) * ring + late_slots(tiles)[1]) * rows * LANES * 4
    slots = late_slots(tiles)[1]
    conserved, faces, late = pl.pallas_call(
        functools.partial(kernel, nrow, nphi, rows, cells, tiles, cycles),
        out_shape=(
            pltpu.VMEM((fields, rows * ring, LANES), f32),
            pltpu.VMEM((nface, rows * ring, LANES), f32),
            pltpu.VMEM((slots, rows, LANES), f32),
        ),
        in_specs=[far, far, far, far],
        out_specs=(near, near, near),
        scratch_shapes=[
            shape(nvar, (rows + 4) * ring, LANES),
            shape(2, nvar, 2, tiles, rows, LANES),
            shape(2, nvar, 2, tiles, rows, LANES),
            shape(tiles, rows, LANES),
            shape(tiles, rows, LANES),
            shape(ring, LANES),
            shape(rows * cells, LANES),
            shape(rows, LANES),
            shape(rows, LANES),
            shape(rows, LANES),
            shape(nphi // 2, rows, LANES),
            shape(2, rows, LANES),
            pltpu.SMEM((2 * cycles,), jnp.int32),
            shape(nvar, theta),
            pltpu.SemaphoreType.DMA((2,)),
            pltpu.SemaphoreType.DMA((fields,)),
            pltpu.SemaphoreType.DMA((2, nvar)),
            pltpu.SemaphoreType.DMA((2, nvar)),
            pltpu.SemaphoreType.DMA,
            pltpu.SemaphoreType.DMA,
            pltpu.SemaphoreType.DMA((nphi // 2,)),
            pltpu.SemaphoreType.DMA((nphi // 2,)),
            pltpu.SemaphoreType.DMA((3,)),
            pltpu.SemaphoreType.DMA((3,)),
            pltpu.SemaphoreType.REGULAR((nphi // 2,)),
            pltpu.SemaphoreType.REGULAR,
            pltpu.SemaphoreType.REGULAR,
        ],
        compiler_params=pltpu.CompilerParams(
            collective_id=0, has_side_effects=True, vmem_limit_bytes=LIMIT - result_bytes
        ),
        name="step",
    )(widths, blocked(hydro_vars), blocked(face_b), diffusion)
    conserved, faces = pl.pallas_call(
        functools.partial(spill, nvar, rows, cells, tiles, cycles),
        out_shape=(
            jax.ShapeDtypeStruct((fields, rows * ring, LANES), f32),
            jax.ShapeDtypeStruct((nface, rows * ring, LANES), f32),
        ),
        in_specs=[near, near, near],
        out_specs=(far, far),
        scratch_shapes=[shape(2, rows * ring, LANES), pltpu.SemaphoreType.DMA((fields + nface,))],
        compiler_params=pltpu.CompilerParams(vmem_limit_bytes=8 * rows * ring * LANES + 2000000),
        name="spill",
    )(conserved, faces, late)
    return unblocked(conserved, rows, cells, theta), unblocked(faces, rows, cells, theta)


def solution(mesh):
    spec = P(None, "row", "phi", None)
    return jax.shard_map(
        functools.partial(body, mesh.shape["row"], mesh.shape["phi"]),
        mesh=mesh,
        in_specs=(spec, spec, P(), P()),
        out_specs=(spec, spec),
        check_vma=False,
    )
```

```python
import functools

import jax
import jax.numpy as jnp
from jax import lax
from jax.experimental import pallas as pl
from jax.experimental.pallas import tpu as pltpu
from jax.sharding import PartitionSpec as P

MESH = pl.DeviceIdType.MESH
LANES = 128
SUB = 8
EARLY = 1
MIDDLE = 2
HELD_NEAR = 2
HELD_FAR = 2
LATE = (0, 1, 2, 3, 4)
LIMIT = 58000000


def late_slots(nvar, tiles):
    names = ("mean_left", "mean_right", "scale", "mean_face", "local", "odd")
    sizes = (nvar, nvar, nvar * tiles, 1, 1, 1)
    starts, total = {}, 0
    for name, size in zip(names, sizes):
        starts[name] = total
        total += size
    return starts, total


def sent_edge(R, way, k, t):
    return R[way, k, 0, t] if k >= MIDDLE else R[way, k + MIDDLE, 1, t]


def fix_polar(low, high, last, raw, edge, t):
    if t == 0:
        raw = jnp.where(low, edge, raw)
    if t == last:
        raw = jnp.where(high, edge, raw)
    return raw


def halo_terms(scale, from_left, from_right, inner):
    l1, l2 = from_left[1] - inner[3], from_left[0] - inner[2]
    r1, r2 = from_right[0] - inner[0], from_right[1] - inner[1]
    return [scale * term for term in (16.0 * l1 - l2, -l1, -r1, 16.0 * r1 - r2)]


def kernel(
    nrow, nphi, rows, cells, tiles, cycles,
    widths_far, hydro, face, diffusion_far, O, F, A, H, R, RF,
    S, SF, FN, Q, M, PX, OM, MG, E,
    widths, diffusion, small_sem, load_sem, send_phi, recv_phi, send_face, recv_face,
    send_mean, recv_mean, send_row, recv_row, pair_ack, far_ack, row_ack,
):
    nvar = hydro.shape[0]
    nface = face.shape[0]
    fields = nvar + nface
    last = tiles - 1
    blocks = cells // SUB
    ring = cells * tiles
    row = lax.axis_index("row")
    phi = lax.axis_index("phi")
    left = lax.rem(phi + nphi - 1, nphi)
    right = lax.rem(phi + 1, nphi)
    pairs = nphi // 2
    pair = phi // 2
    odd = lax.rem(phi, 2)
    partner = phi + 1 - 2 * odd
    far = jnp.where(odd == 1, right, left)
    near_way, far_way = 1 - odd, odd
    yields_near = (phi == 1) & (lax.rem(row, 2) == 1)
    yields_far = (phi == nphi - 1) & (lax.rem(row, 2) == 1)
    packed = 2 * cycles

    loads = [pltpu.make_async_copy(hydro.at[k], H.at[k, pl.ds(2 * ring, rows * ring)], load_sem.at[k]) for k in range(nvar)]
    loads += [pltpu.make_async_copy(face.at[k], F.at[k], load_sem.at[nvar + k]) for k in range(nface)]
    small = [
        pltpu.make_async_copy(widths_far, widths, small_sem.at[0]),
        pltpu.make_async_copy(diffusion_far, diffusion, small_sem.at[1]),
    ]
    for c in small + loads:
        c.start()

    barrier = pltpu.get_barrier_semaphore()

    def greet(**device):
        pl.semaphore_signal(barrier, inc=1, device_id=device, device_id_type=MESH)

    greet(phi=partner)

    @pl.when(far > phi)
    def _():
        greet(phi=far)

    @pl.when(row < nrow - 1)
    def _():
        greet(row=row + 1)

    for step in range(1, pairs):

        @pl.when(pair + step < pairs)
        def _(step=step):
            greet(phi=phi + 2 * step)

    lane = lax.broadcasted_iota(jnp.int32, (1, LANES), 1)
    low = lane < cycles
    high = lane >= LANES - cycles
    mine = [(lane >= packed * f) & (lane < packed * (f + 1)) for f in range(fields)]

    def part(t):
        return slice(t * LANES, (t + 1) * LANES)

    def pack(value, f):
        return pltpu.roll(value, (cycles + packed * f) % LANES, 1)

    def unpack(value, f):
        return pltpu.roll(value, (-(cycles + packed * f)) % LANES, 1)

    def spot(r, b, t):
        start = r * ring + (b * tiles + t) * SUB
        return pl.ds(start if isinstance(r, int) else pl.multiple_of(start, SUB), SUB)

    def layer(r, cell, t):
        return pl.ds(r * ring + (cell // SUB * tiles + t) * SUB + cell % SUB, rows, stride=ring)

    def place(f):
        return (H, f, 2) if f < nvar else (F, f - nvar, 0)

    def halo(way, target, k):
        return pltpu.make_async_remote_copy(
            src_ref=S.at[way, k], dst_ref=R.at[way, k], send_sem=send_phi.at[way, k], recv_sem=recv_phi.at[way, k],
            device_id={"phi": target}, device_id_type=MESH)

    def near_copy(k):
        return halo(near_way, partner, k)

    def far_copy(k):
        return halo(far_way, far, k)

    mean_near = pltpu.make_async_remote_copy(
        src_ref=M, dst_ref=PX, send_sem=send_mean.at[0], recv_sem=recv_mean.at[0],
        device_id={"phi": partner}, device_id_type=MESH)

    def mean_copy(step):
        return pltpu.make_async_remote_copy(
            src_ref=MG.at[pair], dst_ref=MG.at[pair], send_sem=send_mean.at[step], recv_sem=recv_mean.at[step],
            device_id={"phi": lax.rem(phi + 2 * step, nphi)}, device_id_type=MESH)

    def pack_halo(k):
        for t in range(tiles):
            for i in range(2):
                S[0, k, i, t] = H[k, layer(2, i, t), :]
                S[1, k, i, t] = H[k, layer(2, cells - 2 + i, t), :]

    for k in range(nvar):
        loads[k].wait()
        pack_halo(k)
        if k == 0:
            known = 1 + jnp.where(far < phi, 1, 0) + pair + jnp.where(row > 0, 1, 0)
            pl.semaphore_wait(barrier, known)
            for step in range(1, pairs):

                @pl.when(pair >= step)
                def _(step=step):
                    pl.semaphore_signal(pair_ack.at[step], inc=1, device_id={"phi": phi - 2 * step}, device_id_type=MESH)

            @pl.when(far < phi)
            def _():
                pl.semaphore_signal(far_ack, inc=1, device_id={"phi": far}, device_id_type=MESH)

            @pl.when(row > 0)
            def _():
                pl.semaphore_signal(row_ack, inc=1, device_id={"row": row - 1}, device_id_type=MESH)

        if k < EARLY:
            near_copy(k).start()
        if k < MIDDLE:

            @pl.when(phi == nphi - 1)
            def _(k=k):
                far_copy(k).start()

    for c in loads[nvar:]:
        c.wait()
    face_left = pltpu.make_async_remote_copy(
        src_ref=SF, dst_ref=RF, send_sem=send_face, recv_sem=recv_face,
        device_id={"phi": left}, device_id_type=MESH)
    for t in range(tiles):
        SF[t] = F[nface - 1, layer(0, 0, t), :]

    @pl.when(odd == 1)
    def _():
        face_left.start()


    def polar_cells(r, b):
        value = jnp.zeros((SUB, LANES), jnp.float32)
        for f in range(fields):
            ref, k, base = place(f)
            polar = jnp.where(low, ref[k, spot(r + base, b, 0), :], ref[k, spot(r + base, b, last), :])
            value = jnp.where(mine[f], pack(polar, f), value)
        return value

    def cell_mean(r, carry):
        value = jnp.zeros((SUB, LANES), jnp.float32)
        for f in range(fields):
            ref, k, base = place(f)
            sums = [ref[k, spot(r + base, 0, t), :] for t in (0, last)]
            for b in range(1, blocks):
                sums = [x + ref[k, spot(r + base, b, t), :] for x, t in zip(sums, (0, last))]
            value = jnp.where(mine[f], pack(jnp.where(low, sums[0], sums[1]), f), value)
        size = SUB // 2
        while size:
            value = value + pltpu.roll(value, size, 0)
            size //= 2
        M[pl.ds(r, 1), :] = value[0:1] * (1.0 / cells)
        return carry

    lax.fori_loop(0, rows, cell_mean, 0, unroll=4)
    mean_near.start()
    for k in range(EARLY, MIDDLE):
        near_copy(k).start()

    for c in small:
        c.wait()
    width = jnp.zeros((1, LANES), jnp.int32)
    slot = lax.rem(lane, packed)
    for j in range(cycles):
        width = jnp.where(slot == cycles + j, widths[j], width)
        width = jnp.where(slot == j, widths[cycles + j], width)

    index = lax.broadcasted_iota(jnp.int32, (SUB, LANES), 0)

    def local_average(r, carry):
        totals = [polar_cells(r, b) for b in range(blocks)]
        results = list(totals)
        size = 1
        while size < cells:
            if size < SUB:
                turned = []
                for v in totals:
                    forward = pltpu.roll(v, SUB - size, 0)
                    if 2 * size < SUB:
                        forward = jnp.where((index & size) == 0, forward, pltpu.roll(v, size, 0))
                    turned.append(v + forward)
                totals = turned
            else:
                hop = size // SUB
                totals = [totals[b] + totals[b ^ hop] for b in range(blocks)]
            size *= 2
            results = [jnp.where(width == size, v * (1.0 / size), old) for v, old in zip(totals, results)]
        for b in range(blocks):
            Q[pl.ds(pl.multiple_of(r * cells + b * SUB, SUB), SUB), :] = results[b]
        E[0, pl.ds(r, 1), :] = results[0][0:1]
        E[1, pl.ds(r, 1), :] = results[blocks - 1][SUB - 1 : SUB]
        return carry

    lax.fori_loop(0, rows, local_average, 0, unroll=2)

    def put_edges(way, k, i, f, source):
        edges = unpack(E[source], f)
        S[way, k, i, 0] = jnp.where(low, edges, S[way, k, i, 0])
        S[way, k, i, last] = jnp.where(high, edges, S[way, k, i, last])

    for k in range(MIDDLE, nvar):
        for way in range(2):
            put_edges(way, k, 0, k, way)
            if k < 2 * MIDDLE:
                put_edges(way, k, 1, k - MIDDLE, way)
    put_edges(0, nvar - 1, 1, fields - 1, 0)

    for k in range(MIDDLE, HELD_NEAR):
        near_copy(k).start()

    @pl.when(jnp.logical_not(yields_near))
    def _():
        for k in range(HELD_NEAR, nvar):
            near_copy(k).start()


    mean_near.wait_recv()
    MG[pair] = (M[...] + PX[...]) * 0.5
    for step in range(1, pairs):

        @pl.when(pair + step < pairs)
        def _(step=step):
            pl.semaphore_wait(pair_ack.at[step], 1)

        mean_copy(step).start()

    def start_far():
        @pl.when(far > phi)
        def _():
            pl.semaphore_wait(far_ack, 1)

        @pl.when(odd == 0)
        def _():
            edges = unpack(E[0], fields - 1)
            SF[0] = jnp.where(low, edges, SF[0])
            SF[last] = jnp.where(high, edges, SF[last])
            face_left.start()

        @pl.when(phi < nphi - 1)
        def _():
            for k in range(MIDDLE):
                far_copy(k).start()

        for k in range(MIDDLE, HELD_FAR):
            far_copy(k).start()

        @pl.when(jnp.logical_not(yields_far))
        def _():
            for k in range(HELD_FAR, nvar):
                far_copy(k).start()

    @pl.when(phi > 0)
    def _():
        start_far()

    for step in range(pairs - 1, 1, -1):
        mean_copy(step).wait_recv()

    @pl.when(phi == 0)
    def _():
        start_far()

    mean_copy(1).wait_recv()

    def group_mean(who):
        result = MG[who // 2]
        size = 2
        while size <= pairs:
            start = (who // (2 * size)) * size
            total = MG[start]
            for i in range(1, size):
                total = total + MG[start + i]
            result = jnp.where(width == 2 * size * cells, total * (1.0 / size), result)
            size *= 2
        return result

    OM[...] = group_mean(phi)
    next_lo = group_mean(right)
    next_hi = group_mean(left)
    wide = width > cells

    def spread(r):
        mean = jnp.broadcast_to(OM[pl.ds(r, 1), :], (SUB, LANES))
        for b in range(blocks):
            where = pl.ds(r * cells + b * SUB if isinstance(r, int) else pl.multiple_of(r * cells + b * SUB, SUB), SUB)
            value = jnp.where(wide, mean, Q[where, :])
            for f in range(fields):
                ref, k, base = place(f)
                polar = unpack(value, f)
                ref[k, spot(r + base, b, 0), :] = jnp.where(low, polar, ref[k, spot(r + base, b, 0), :])
                ref[k, spot(r + base, b, last), :] = jnp.where(high, polar, ref[k, spot(r + base, b, last), :])

    for r in (0, 1, rows - 2, rows - 1):
        spread(r)

    down = pltpu.make_async_remote_copy(
        src_ref=H.at[:, pl.ds(2 * ring, 2 * ring)], dst_ref=H.at[:, pl.ds((rows + 2) * ring, 2 * ring)],
        send_sem=send_row.at[0], recv_sem=recv_row.at[0], device_id={"row": row - 1}, device_id_type=MESH)
    down_face = pltpu.make_async_remote_copy(
        src_ref=F.at[0, pl.ds(0, ring)], dst_ref=FN,
        send_sem=send_row.at[1], recv_sem=recv_row.at[1], device_id={"row": row - 1}, device_id_type=MESH)
    up = pltpu.make_async_remote_copy(
        src_ref=H.at[:, pl.ds(rows * ring, 2 * ring)], dst_ref=H.at[:, pl.ds(0, 2 * ring)],
        send_sem=send_row.at[2], recv_sem=recv_row.at[2], device_id={"row": row + 1}, device_id_type=MESH)

    @pl.when(row > 0)
    def _():
        down.start()
        down_face.start()

    @pl.when(row < nrow - 1)
    def _():
        pl.semaphore_wait(row_ack, 1)
        up.start()

    lax.fori_loop(2, rows - 2, lambda r, c: (spread(r), c)[1], 0, unroll=4)

    @pl.when(yields_near)
    def _():
        for k in range(HELD_NEAR, nvar):
            near_copy(k).start()

    @pl.when(yields_far)
    def _():
        for k in range(HELD_FAR, nvar):
            far_copy(k).start()

    @pl.when(row == 0)
    def _():
        H[:, pl.ds(0, 2 * ring), :] = jnp.zeros((nvar, 2 * ring, LANES), jnp.float32)

    @pl.when(row == nrow - 1)
    def _():
        H[:, pl.ds((rows + 2) * ring, 2 * ring), :] = jnp.zeros((nvar, 2 * ring, LANES), jnp.float32)
        FN[...] = jnp.zeros_like(FN)

    def whole(ref, k, r, t):
        return jnp.concatenate([ref[k, spot(r, b, t), :] for b in range(blocks)], 0)

    def write(k, r, t, value):
        for b in range(blocks):
            O[k, spot(r, b, t), :] = value[b * SUB : (b + 1) * SUB]

    def shifted(parts, amount):
        out = []
        turned = [pltpu.roll(p, (-amount) % LANES, 1) for p in parts]
        for t in range(tiles):
            if amount > 0:
                inside = lane < LANES - amount
                other = turned[t + 1] if t + 1 < tiles else 0.0
            else:
                inside = lane >= -amount
                other = turned[t - 1] if t > 0 else 0.0
            out.append(jnp.where(inside, turned[t], other))
        return out

    def smooth_row(r):
        for k in range(nvar):
            mid = [whole(H, k, r + 2, t) for t in range(tiles)]
            one = [a + b for a, b in zip(shifted(mid, 1), shifted(mid, -1))]
            two = [a + b for a, b in zip(shifted(mid, 2), shifted(mid, -2))]
            for t in range(tiles):
                v = mid[t]
                s1 = one[t] + (pltpu.roll(v, 1, 0) + pltpu.roll(v, cells - 1, 0)) + (whole(H, k, r + 1, t) + whole(H, k, r + 3, t))
                s2 = two[t] + (pltpu.roll(v, 2, 0) + pltpu.roll(v, cells - 2, 0)) + (whole(H, k, r, t) + whole(H, k, r + 4, t))
                change = (16.0 * s1 - s2 - 90.0 * v) * (1.0 / 12.0)
                write(k, r, t, v + diffusion[k : k + 1, part(t)] * change)

    def field_row(r, following):
        polar = [whole(F, 1, r, t) for t in range(tiles)]
        polar_next = shifted(polar, 1)
        for t in range(tiles):
            write(nvar, r, t, 0.5 * (whole(F, 0, r, t) + following(t)))
            write(nvar + 1, r, t, 0.5 * (polar[t] + polar_next[t]))
            azimuth = whole(F, 2, r, t)
            write(nvar + 2, r, t, 0.5 * (azimuth + pltpu.roll(azimuth, cells - 1, 0)))

    def inner_row(r, carry):
        field_row(r, lambda t: whole(F, 0, r + 1, t))
        smooth_row(r)
        return carry

    lax.fori_loop(2, rows - 2, inner_row, 0, unroll=4)
    for r in (0, 1, rows - 2):
        field_row(r, lambda t, r=r: whole(F, 0, r + 1, t))

    @pl.when(row > 0)
    def _():
        up.wait_recv()

    @pl.when(row < nrow - 1)
    def _():
        down.wait_recv()
        down_face.wait_recv()

    field_row(rows - 1, lambda t: jnp.concatenate([FN[spot(0, b, t), :] for b in range(blocks)], 0))
    for r in (0, 1, rows - 2, rows - 1):
        smooth_row(r)

    local = unpack(width, 0) <= cells
    ends = (0, 1, cells - 2, cells - 1)

    def patch(k):
        mean_l = unpack(next_hi, k)
        mean_r = unpack(next_lo, k)
        for t in range(tiles):
            edge_l = jnp.where(local, sent_edge(R, 1, k, t), mean_l)
            edge_r = jnp.where(local, sent_edge(R, 0, k, t), mean_r)
            terms = halo_terms(
                diffusion[k : k + 1, part(t)] * (1.0 / 12.0),
                [fix_polar(low, high, last, R[1, k, i, t], edge_l, t) for i in range(2)],
                [fix_polar(low, high, last, R[0, k, i, t], edge_r, t) for i in range(2)],
                [H[k, layer(2, cell, t), :] for cell in ends])
            for cell, term in zip(ends, terms):
                O[k, layer(0, cell, t), :] = O[k, layer(0, cell, t), :] + term

    def arrive(k):
        halo(1, right, k).wait_recv()
        halo(0, left, k).wait_recv()

    slots, _ = late_slots(nvar, tiles)
    for k in range(nvar):
        if k in LATE:
            A[slots["mean_left"] + k] = unpack(next_hi, k)
            A[slots["mean_right"] + k] = unpack(next_lo, k)
            for t in range(tiles):
                A[slots["scale"] + k * tiles + t] = jnp.broadcast_to(
                    diffusion[k : k + 1, part(t)] * (1.0 / 12.0), (rows, LANES))
    A[slots["mean_face"]] = unpack(next_lo, fields - 1)
    A[slots["local"]] = jnp.broadcast_to(jnp.where(local, 1.0, 0.0), (rows, LANES))
    A[slots["odd"]] = jnp.full((rows, LANES), odd, jnp.int32).astype(jnp.float32)
    for k in range(MIDDLE):
        arrive(k)
    face_left.wait_recv()
    for k in range(MIDDLE, nvar):
        arrive(k)
        for n in (k - MIDDLE, k):
            if n not in LATE and (n < MIDDLE or n == k):
                patch(n)

    for k in range(nvar):
        near_copy(k).wait_send()
        far_copy(k).wait_send()
    face_left.wait_send()
    mean_near.wait_send()
    for step in range(1, pairs):
        mean_copy(step).wait_send()

    @pl.when(row > 0)
    def _():
        down.wait_send()
        down_face.wait_send()

    @pl.when(row < nrow - 1)
    def _():
        up.wait_send()


def spill(nvar, rows, cells, tiles, cycles, conserved, faces, A, H, R, RF, conserved_out, faces_out, P, sem):
    fields = conserved.shape[0]
    nface = faces.shape[0]
    ring = cells * tiles
    last = tiles - 1
    late = LATE + (fields - 1,)

    def layer(r, cell, t):
        return pl.ds(r * ring + (cell // SUB * tiles + t) * SUB + cell % SUB, rows, stride=ring)

    def out(k, source):
        return pltpu.make_async_copy(source, conserved_out.at[k], sem.at[k])

    copies = [pltpu.make_async_copy(faces.at[k], faces_out.at[k], sem.at[fields + k]) for k in range(nface)]
    copies += [out(k, conserved.at[k]) for k in range(fields) if k not in late]
    for c in copies:
        c.start()

    slots, _ = late_slots(nvar, tiles)
    lane = lax.broadcasted_iota(jnp.int32, (1, LANES), 1)
    low = lane < cycles
    high = lane >= LANES - cycles
    local = A[slots["local"]] > 0.5
    odd = A[slots["odd"]] > 0.5
    ends = (0, 1, cells - 2, cells - 1)
    slot = len(LATE)
    P[slot] = conserved[fields - 1]
    for t in range(tiles):
        edge = jnp.where(odd, RF[t], R[0, nvar - 1, 1, t])
        edge = jnp.where(local, edge, A[slots["mean_face"]])
        following = fix_polar(low, high, last, RF[t], edge, t)
        P[slot, layer(0, cells - 1, t), :] = 0.5 * (faces[nface - 1, layer(0, cells - 1, t), :] + following)
    copies.append(out(fields - 1, P.at[slot]))
    copies[-1].start()
    for n, k in enumerate(LATE):
        P[n] = conserved[k]
        for t in range(tiles):
            edge_l = jnp.where(local, sent_edge(R, 1, k, t), A[slots["mean_left"] + k])
            edge_r = jnp.where(local, sent_edge(R, 0, k, t), A[slots["mean_right"] + k])
            terms = halo_terms(
                A[slots["scale"] + k * tiles + t],
                [fix_polar(low, high, last, R[1, k, i, t], edge_l, t) for i in range(2)],
                [fix_polar(low, high, last, R[0, k, i, t], edge_r, t) for i in range(2)],
                [H[k, layer(2, cell, t), :] for cell in ends])
            for cell, term in zip(ends, terms):
                P[n, layer(0, cell, t), :] = P[n, layer(0, cell, t), :] + term
        copies.append(out(k, P.at[n]))
        copies[-1].start()
    for c in copies:
        c.wait()


def blocked(x):
    n, rows, cells, theta = x.shape
    x = x.reshape(n, rows, cells // SUB, SUB, theta // LANES, LANES)
    return x.transpose(0, 1, 2, 4, 3, 5).reshape(n, rows * cells * (theta // LANES), LANES)


def unblocked(x, rows, cells, theta):
    x = x.reshape(x.shape[0], rows, cells // SUB, theta // LANES, SUB, LANES)
    return x.transpose(0, 1, 2, 4, 3, 5).reshape(x.shape[0], rows, cells, theta)


def body(nrow, nphi, hydro_vars, face_b, widths, diffusion):
    nvar, rows, cells, theta = hydro_vars.shape
    nface = face_b.shape[0]
    fields = nvar + nface
    cycles = widths.shape[0] // 2
    tiles = theta // LANES
    ring = cells * tiles
    f32 = jnp.float32
    shape = lambda *s: pltpu.VMEM(s, f32)
    far = pl.BlockSpec(memory_space=pltpu.HBM)
    near = pl.BlockSpec(memory_space=pltpu.VMEM)
    slots = late_slots(nvar, tiles)[1]
    held = ((fields + nface) * rows + nvar * (rows + 4)) * ring + (slots + (4 * nvar + 1) * tiles) * rows
    result_bytes = held * LANES * 4
    conserved, faces, *late = pl.pallas_call(
        functools.partial(kernel, nrow, nphi, rows, cells, tiles, cycles),
        out_shape=(
            pltpu.VMEM((fields, rows * ring, LANES), f32),
            pltpu.VMEM((nface, rows * ring, LANES), f32),
            pltpu.VMEM((slots, rows, LANES), f32),
            shape(nvar, (rows + 4) * ring, LANES),
            shape(2, nvar, 2, tiles, rows, LANES),
            shape(tiles, rows, LANES),
        ),
        in_specs=[far, far, far, far],
        out_specs=(near,) * 6,
        scratch_shapes=[
            shape(2, nvar, 2, tiles, rows, LANES),
            shape(tiles, rows, LANES),
            shape(ring, LANES),
            shape(rows * cells, LANES),
            shape(rows, LANES),
            shape(rows, LANES),
            shape(rows, LANES),
            shape(nphi // 2, rows, LANES),
            shape(2, rows, LANES),
            pltpu.SMEM((2 * cycles,), jnp.int32),
            shape(nvar, theta),
            pltpu.SemaphoreType.DMA((2,)),
            pltpu.SemaphoreType.DMA((fields,)),
            pltpu.SemaphoreType.DMA((2, nvar)),
            pltpu.SemaphoreType.DMA((2, nvar)),
            pltpu.SemaphoreType.DMA,
            pltpu.SemaphoreType.DMA,
            pltpu.SemaphoreType.DMA((nphi // 2,)),
            pltpu.SemaphoreType.DMA((nphi // 2,)),
            pltpu.SemaphoreType.DMA((3,)),
            pltpu.SemaphoreType.DMA((3,)),
            pltpu.SemaphoreType.REGULAR((nphi // 2,)),
            pltpu.SemaphoreType.REGULAR,
            pltpu.SemaphoreType.REGULAR,
        ],
        compiler_params=pltpu.CompilerParams(
            collective_id=0, has_side_effects=True, vmem_limit_bytes=LIMIT - result_bytes
        ),
        name="step",
    )(widths, blocked(hydro_vars), blocked(face_b), diffusion)
    conserved, faces = pl.pallas_call(
        functools.partial(spill, nvar, rows, cells, tiles, cycles),
        out_shape=(
            jax.ShapeDtypeStruct((fields, rows * ring, LANES), f32),
            jax.ShapeDtypeStruct((nface, rows * ring, LANES), f32),
        ),
        in_specs=[near] * 6,
        out_specs=(far, far),
        scratch_shapes=[shape(len(LATE) + 1, rows * ring, LANES), pltpu.SemaphoreType.DMA((fields + nface,))],
        compiler_params=pltpu.CompilerParams(vmem_limit_bytes=4 * (len(LATE) + 1) * rows * ring * LANES + 2000000),
        name="spill",
    )(conserved, faces, *late)
    return unblocked(conserved, rows, cells, theta), unblocked(faces, rows, cells, theta)


def solution(mesh):
    spec = P(None, "row", "phi", None)
    return jax.shard_map(
        functools.partial(body, mesh.shape["row"], mesh.shape["phi"]),
        mesh=mesh,
        in_specs=(spec, spec, P(), P()),
        out_specs=(spec, spec),
        check_vma=False,
    )
```

```python
import functools

import jax
import jax.numpy as jnp
from jax import lax
from jax.experimental import pallas as pl
from jax.experimental.pallas import tpu as pltpu
from jax.sharding import PartitionSpec as P

MESH = pl.DeviceIdType.MESH
LANES = 128
SUB = 8
EARLY = 1
MIDDLE = 2
HELD_NEAR = 2
HELD_FAR = 2
LIMIT = 58000000


def late_slots(nvar, tiles):
    names = ("mean_left", "mean_right", "scale", "mean_face", "local", "odd")
    sizes = (nvar, nvar, nvar * tiles, 1, 1, 1)
    starts, total = {}, 0
    for name, size in zip(names, sizes):
        starts[name] = total
        total += size
    return starts, total


def sent_edge(R, way, k, t):
    early = k < MIDDLE
    return R[way, jnp.where(early, k + MIDDLE, k), jnp.where(early, 1, 0), t]


def fix_polar(low, high, last, raw, edge, t):
    if t == 0:
        raw = jnp.where(low, edge, raw)
    if t == last:
        raw = jnp.where(high, edge, raw)
    return raw


def halo_terms(scale, from_left, from_right, inner):
    l1, l2 = from_left[1] - inner[3], from_left[0] - inner[2]
    r1, r2 = from_right[0] - inner[0], from_right[1] - inner[1]
    return [scale * term for term in (16.0 * l1 - l2, -l1, -r1, 16.0 * r1 - r2)]


def kernel(
    nrow, nphi, rows, cells, tiles, cycles,
    widths_far, hydro, face, diffusion_far, O, F, A, H, R, RF,
    S, SF, FN, Q, M, PX, OM, MG, E,
    widths, diffusion, small_sem, load_sem, send_phi, recv_phi, send_face, recv_face,
    send_mean, recv_mean, send_row, recv_row, pair_ack, far_ack, row_ack,
):
    nvar = hydro.shape[0]
    nface = face.shape[0]
    fields = nvar + nface
    last = tiles - 1
    blocks = cells // SUB
    ring = cells * tiles
    row = lax.axis_index("row")
    phi = lax.axis_index("phi")
    left = lax.rem(phi + nphi - 1, nphi)
    right = lax.rem(phi + 1, nphi)
    pairs = nphi // 2
    pair = phi // 2
    odd = lax.rem(phi, 2)
    partner = phi + 1 - 2 * odd
    far = jnp.where(odd == 1, right, left)
    near_way, far_way = 1 - odd, odd
    yields_near = (phi == 1) & (lax.rem(row, 2) == 1)
    yields_far = (phi == nphi - 1) & (lax.rem(row, 2) == 1)
    packed = 2 * cycles

    loads = [pltpu.make_async_copy(hydro.at[k], H.at[k, pl.ds(2 * ring, rows * ring)], load_sem.at[k]) for k in range(nvar)]
    loads += [pltpu.make_async_copy(face.at[k], F.at[k], load_sem.at[nvar + k]) for k in range(nface)]
    small = [
        pltpu.make_async_copy(widths_far, widths, small_sem.at[0]),
        pltpu.make_async_copy(diffusion_far, diffusion, small_sem.at[1]),
    ]
    for c in small + loads:
        c.start()

    barrier = pltpu.get_barrier_semaphore()

    def greet(**device):
        pl.semaphore_signal(barrier, inc=1, device_id=device, device_id_type=MESH)

    greet(phi=partner)

    @pl.when(far > phi)
    def _():
        greet(phi=far)

    @pl.when(row < nrow - 1)
    def _():
        greet(row=row + 1)

    for step in range(1, pairs):

        @pl.when(pair + step < pairs)
        def _(step=step):
            greet(phi=phi + 2 * step)

    lane = lax.broadcasted_iota(jnp.int32, (1, LANES), 1)
    low = lane < cycles
    high = lane >= LANES - cycles
    mine = [(lane >= packed * f) & (lane < packed * (f + 1)) for f in range(fields)]

    def part(t):
        return slice(t * LANES, (t + 1) * LANES)

    def pack(value, f):
        return pltpu.roll(value, (cycles + packed * f) % LANES, 1)

    def unpack(value, f):
        return pltpu.roll(value, (-(cycles + packed * f)) % LANES, 1)

    def spot(r, b, t):
        start = r * ring + (b * tiles + t) * SUB
        return pl.ds(start if isinstance(r, int) else pl.multiple_of(start, SUB), SUB)

    def layer(r, cell, t):
        return pl.ds(r * ring + (cell // SUB * tiles + t) * SUB + cell % SUB, rows, stride=ring)

    def place(f):
        return (H, f, 2) if f < nvar else (F, f - nvar, 0)

    def halo(way, target, k):
        return pltpu.make_async_remote_copy(
            src_ref=S.at[way, k], dst_ref=R.at[way, k], send_sem=send_phi.at[way, k], recv_sem=recv_phi.at[way, k],
            device_id={"phi": target}, device_id_type=MESH)

    def near_copy(k):
        return halo(near_way, partner, k)

    def far_copy(k):
        return halo(far_way, far, k)

    mean_near = pltpu.make_async_remote_copy(
        src_ref=M, dst_ref=PX, send_sem=send_mean.at[0], recv_sem=recv_mean.at[0],
        device_id={"phi": partner}, device_id_type=MESH)

    def mean_copy(step):
        return pltpu.make_async_remote_copy(
            src_ref=MG.at[pair], dst_ref=MG.at[pair], send_sem=send_mean.at[step], recv_sem=recv_mean.at[step],
            device_id={"phi": lax.rem(phi + 2 * step, nphi)}, device_id_type=MESH)

    def pack_halo(k):
        for t in range(tiles):
            for i in range(2):
                S[0, k, i, t] = H[k, layer(2, i, t), :]
                S[1, k, i, t] = H[k, layer(2, cells - 2 + i, t), :]

    for k in range(nvar):
        loads[k].wait()
        pack_halo(k)
        if k == 0:
            known = 1 + jnp.where(far < phi, 1, 0) + pair + jnp.where(row > 0, 1, 0)
            pl.semaphore_wait(barrier, known)
            for step in range(1, pairs):

                @pl.when(pair >= step)
                def _(step=step):
                    pl.semaphore_signal(pair_ack.at[step], inc=1, device_id={"phi": phi - 2 * step}, device_id_type=MESH)

            @pl.when(far < phi)
            def _():
                pl.semaphore_signal(far_ack, inc=1, device_id={"phi": far}, device_id_type=MESH)

            @pl.when(row > 0)
            def _():
                pl.semaphore_signal(row_ack, inc=1, device_id={"row": row - 1}, device_id_type=MESH)

        if k < EARLY:
            near_copy(k).start()
        if k < MIDDLE:

            @pl.when(phi == nphi - 1)
            def _(k=k):
                far_copy(k).start()

    for c in loads[nvar:]:
        c.wait()
    face_left = pltpu.make_async_remote_copy(
        src_ref=SF, dst_ref=RF, send_sem=send_face, recv_sem=recv_face,
        device_id={"phi": left}, device_id_type=MESH)
    for t in range(tiles):
        SF[t] = F[nface - 1, layer(0, 0, t), :]

    @pl.when(odd == 1)
    def _():
        face_left.start()


    def polar_cells(r, b):
        value = jnp.zeros((SUB, LANES), jnp.float32)
        for f in range(fields):
            ref, k, base = place(f)
            polar = jnp.where(low, ref[k, spot(r + base, b, 0), :], ref[k, spot(r + base, b, last), :])
            value = jnp.where(mine[f], pack(polar, f), value)
        return value

    def cell_mean(r, carry):
        value = jnp.zeros((SUB, LANES), jnp.float32)
        for f in range(fields):
            ref, k, base = place(f)
            sums = [ref[k, spot(r + base, 0, t), :] for t in (0, last)]
            for b in range(1, blocks):
                sums = [x + ref[k, spot(r + base, b, t), :] for x, t in zip(sums, (0, last))]
            value = jnp.where(mine[f], pack(jnp.where(low, sums[0], sums[1]), f), value)
        size = SUB // 2
        while size:
            value = value + pltpu.roll(value, size, 0)
            size //= 2
        M[pl.ds(r, 1), :] = value[0:1] * (1.0 / cells)
        return carry

    lax.fori_loop(0, rows, cell_mean, 0, unroll=8)
    mean_near.start()
    for k in range(EARLY, MIDDLE):
        near_copy(k).start()

    for c in small:
        c.wait()
    width = jnp.zeros((1, LANES), jnp.int32)
    slot = lax.rem(lane, packed)
    for j in range(cycles):
        width = jnp.where(slot == cycles + j, widths[j], width)
        width = jnp.where(slot == j, widths[cycles + j], width)

    index = lax.broadcasted_iota(jnp.int32, (SUB, LANES), 0)

    def local_average(r, carry):
        totals = [polar_cells(r, b) for b in range(blocks)]
        results = list(totals)
        size = 1
        while size < cells:
            if size < SUB:
                turned = []
                for v in totals:
                    forward = pltpu.roll(v, SUB - size, 0)
                    if 2 * size < SUB:
                        forward = jnp.where((index & size) == 0, forward, pltpu.roll(v, size, 0))
                    turned.append(v + forward)
                totals = turned
            else:
                hop = size // SUB
                totals = [totals[b] + totals[b ^ hop] for b in range(blocks)]
            size *= 2
            results = [jnp.where(width == size, v * (1.0 / size), old) for v, old in zip(totals, results)]
        for b in range(blocks):
            Q[pl.ds(pl.multiple_of(r * cells + b * SUB, SUB), SUB), :] = results[b]
        E[0, pl.ds(r, 1), :] = results[0][0:1]
        E[1, pl.ds(r, 1), :] = results[blocks - 1][SUB - 1 : SUB]
        return carry

    lax.fori_loop(0, rows, local_average, 0, unroll=4)

    def put_edges(way, k, i, f, source):
        edges = unpack(E[source], f)
        S[way, k, i, 0] = jnp.where(low, edges, S[way, k, i, 0])
        S[way, k, i, last] = jnp.where(high, edges, S[way, k, i, last])

    for k in range(MIDDLE, nvar):
        for way in range(2):
            put_edges(way, k, 0, k, way)
            if k < 2 * MIDDLE:
                put_edges(way, k, 1, k - MIDDLE, way)
    put_edges(0, nvar - 1, 1, fields - 1, 0)

    for k in range(MIDDLE, HELD_NEAR):
        near_copy(k).start()

    @pl.when(jnp.logical_not(yields_near))
    def _():
        for k in range(HELD_NEAR, nvar):
            near_copy(k).start()


    mean_near.wait_recv()
    MG[pair] = (M[...] + PX[...]) * 0.5
    for step in range(1, pairs):

        @pl.when(pair + step < pairs)
        def _(step=step):
            pl.semaphore_wait(pair_ack.at[step], 1)

        mean_copy(step).start()

    def start_far():
        @pl.when(far > phi)
        def _():
            pl.semaphore_wait(far_ack, 1)

        @pl.when(odd == 0)
        def _():
            edges = unpack(E[0], fields - 1)
            SF[0] = jnp.where(low, edges, SF[0])
            SF[last] = jnp.where(high, edges, SF[last])
            face_left.start()

        @pl.when(phi < nphi - 1)
        def _():
            for k in range(MIDDLE):
                far_copy(k).start()

        for k in range(MIDDLE, HELD_FAR):
            far_copy(k).start()

        @pl.when(jnp.logical_not(yields_far))
        def _():
            for k in range(HELD_FAR, nvar):
                far_copy(k).start()

    @pl.when(phi > 0)
    def _():
        start_far()

    for step in range(pairs - 1, 0, -1):
        mean_copy(step).wait_recv()
        if step == pairs - 1:

            @pl.when(phi == 0)
            def _():
                start_far()


    def group_mean(who):
        result = MG[who // 2]
        size = 2
        while size <= pairs:
            start = (who // (2 * size)) * size
            total = MG[start]
            for i in range(1, size):
                total = total + MG[start + i]
            result = jnp.where(width == 2 * size * cells, total * (1.0 / size), result)
            size *= 2
        return result

    OM[...] = group_mean(phi)
    next_lo = group_mean(right)
    next_hi = group_mean(left)
    wide = width > cells

    def spread(r):
        mean = jnp.broadcast_to(OM[pl.ds(r, 1), :], (SUB, LANES))
        for b in range(blocks):
            where = pl.ds(r * cells + b * SUB if isinstance(r, int) else pl.multiple_of(r * cells + b * SUB, SUB), SUB)
            value = jnp.where(wide, mean, Q[where, :])
            for f in range(fields):
                ref, k, base = place(f)
                polar = unpack(value, f)
                ref[k, spot(r + base, b, 0), :] = jnp.where(low, polar, ref[k, spot(r + base, b, 0), :])
                ref[k, spot(r + base, b, last), :] = jnp.where(high, polar, ref[k, spot(r + base, b, last), :])

    for r in (0, 1, rows - 2, rows - 1):
        spread(r)

    down = pltpu.make_async_remote_copy(
        src_ref=H.at[:, pl.ds(2 * ring, 2 * ring)], dst_ref=H.at[:, pl.ds((rows + 2) * ring, 2 * ring)],
        send_sem=send_row.at[0], recv_sem=recv_row.at[0], device_id={"row": row - 1}, device_id_type=MESH)
    down_face = pltpu.make_async_remote_copy(
        src_ref=F.at[0, pl.ds(0, ring)], dst_ref=FN,
        send_sem=send_row.at[1], recv_sem=recv_row.at[1], device_id={"row": row - 1}, device_id_type=MESH)
    up = pltpu.make_async_remote_copy(
        src_ref=H.at[:, pl.ds(rows * ring, 2 * ring)], dst_ref=H.at[:, pl.ds(0, 2 * ring)],
        send_sem=send_row.at[2], recv_sem=recv_row.at[2], device_id={"row": row + 1}, device_id_type=MESH)

    @pl.when(row > 0)
    def _():
        down.start()
        down_face.start()

    @pl.when(row < nrow - 1)
    def _():
        pl.semaphore_wait(row_ack, 1)
        up.start()

    lax.fori_loop(2, rows - 2, lambda r, c: (spread(r), c)[1], 0, unroll=4)

    @pl.when(yields_near)
    def _():
        for k in range(HELD_NEAR, nvar):
            near_copy(k).start()

    @pl.when(yields_far)
    def _():
        for k in range(HELD_FAR, nvar):
            far_copy(k).start()

    @pl.when(row == 0)
    def _():
        H[:, pl.ds(0, 2 * ring), :] = jnp.zeros((nvar, 2 * ring, LANES), jnp.float32)

    @pl.when(row == nrow - 1)
    def _():
        H[:, pl.ds((rows + 2) * ring, 2 * ring), :] = jnp.zeros((nvar, 2 * ring, LANES), jnp.float32)
        FN[...] = jnp.zeros_like(FN)

    def whole(ref, k, r, t):
        return jnp.concatenate([ref[k, spot(r, b, t), :] for b in range(blocks)], 0)

    def write(k, r, t, value):
        for b in range(blocks):
            O[k, spot(r, b, t), :] = value[b * SUB : (b + 1) * SUB]

    def shifted(parts, amount):
        out = []
        turned = [pltpu.roll(p, (-amount) % LANES, 1) for p in parts]
        for t in range(tiles):
            if amount > 0:
                inside = lane < LANES - amount
                other = turned[t + 1] if t + 1 < tiles else 0.0
            else:
                inside = lane >= -amount
                other = turned[t - 1] if t > 0 else 0.0
            out.append(jnp.where(inside, turned[t], other))
        return out

    def smooth_row(r):
        for k in range(nvar):
            mid = [whole(H, k, r + 2, t) for t in range(tiles)]
            one = [a + b for a, b in zip(shifted(mid, 1), shifted(mid, -1))]
            two = [a + b for a, b in zip(shifted(mid, 2), shifted(mid, -2))]
            for t in range(tiles):
                v = mid[t]
                s1 = one[t] + (pltpu.roll(v, 1, 0) + pltpu.roll(v, cells - 1, 0)) + (whole(H, k, r + 1, t) + whole(H, k, r + 3, t))
                s2 = two[t] + (pltpu.roll(v, 2, 0) + pltpu.roll(v, cells - 2, 0)) + (whole(H, k, r, t) + whole(H, k, r + 4, t))
                change = (16.0 * s1 - s2 - 90.0 * v) * (1.0 / 12.0)
                write(k, r, t, v + diffusion[k : k + 1, part(t)] * change)

    def field_row(r, following):
        polar = [whole(F, 1, r, t) for t in range(tiles)]
        polar_next = shifted(polar, 1)
        for t in range(tiles):
            write(nvar, r, t, 0.5 * (whole(F, 0, r, t) + following(t)))
            write(nvar + 1, r, t, 0.5 * (polar[t] + polar_next[t]))
            azimuth = whole(F, 2, r, t)
            write(nvar + 2, r, t, 0.5 * (azimuth + pltpu.roll(azimuth, cells - 1, 0)))

    def inner_row(r, carry):
        field_row(r, lambda t: whole(F, 0, r + 1, t))
        smooth_row(r)
        return carry

    lax.fori_loop(2, rows - 2, inner_row, 0, unroll=4)
    for r in (0, 1, rows - 2):
        field_row(r, lambda t, r=r: whole(F, 0, r + 1, t))

    @pl.when(row > 0)
    def _():
        up.wait_recv()

    @pl.when(row < nrow - 1)
    def _():
        down.wait_recv()
        down_face.wait_recv()

    field_row(rows - 1, lambda t: jnp.concatenate([FN[spot(0, b, t), :] for b in range(blocks)], 0))
    for r in (0, 1, rows - 2, rows - 1):
        smooth_row(r)

    local = unpack(width, 0) <= cells

    def arrive(k):
        halo(1, right, k).wait_recv()
        halo(0, left, k).wait_recv()

    slots, _ = late_slots(nvar, tiles)
    for k in range(nvar):
        A[slots["mean_left"] + k] = unpack(next_hi, k)
        A[slots["mean_right"] + k] = unpack(next_lo, k)
        for t in range(tiles):
            A[slots["scale"] + k * tiles + t] = jnp.broadcast_to(
                diffusion[k : k + 1, part(t)] * (1.0 / 12.0), (rows, LANES))
    A[slots["mean_face"]] = unpack(next_lo, fields - 1)
    A[slots["local"]] = jnp.broadcast_to(jnp.where(local, 1.0, 0.0), (rows, LANES))
    A[slots["odd"]] = jnp.full((rows, LANES), odd, jnp.int32).astype(jnp.float32)
    for k in range(MIDDLE):
        arrive(k)
    face_left.wait_recv()
    for k in range(MIDDLE, nvar - 1):
        arrive(k)
    for k in range(nvar):
        if k < nvar - 1:
            near_copy(k).wait_send()
        far_copy(k).wait_send()
    face_left.wait_send()
    mean_near.wait_send()
    for step in range(1, pairs):
        mean_copy(step).wait_send()

    @pl.when(row > 0)
    def _():
        down.wait_send()
        down_face.wait_send()

    @pl.when(row < nrow - 1)
    def _():
        up.wait_send()
    arrive(nvar - 1)
    near_copy(nvar - 1).wait_send()


def spill(nvar, rows, cells, tiles, cycles, conserved, faces, A, H, R, RF, conserved_out, faces_out, P, sem):
    fields = conserved.shape[0]
    nface = faces.shape[0]
    ring = cells * tiles
    last = tiles - 1
    late = tuple(range(nvar)) + (fields - 1,)

    def layer(r, cell, t):
        return pl.ds(r * ring + (cell // SUB * tiles + t) * SUB + cell % SUB, rows, stride=ring)

    def out(k, source):
        return pltpu.make_async_copy(source, conserved_out.at[k], sem.at[k])

    copies = [pltpu.make_async_copy(faces.at[k], faces_out.at[k], sem.at[fields + k]) for k in range(nface)]
    copies += [out(k, conserved.at[k]) for k in range(fields) if k not in late]
    for c in copies:
        c.start()

    slots, _ = late_slots(nvar, tiles)
    lane = lax.broadcasted_iota(jnp.int32, (1, LANES), 1)
    low = lane < cycles
    high = lane >= LANES - cycles
    local = A[slots["local"]] > 0.5
    odd = A[slots["odd"]] > 0.5
    ends = (0, 1, cells - 2, cells - 1)
    slot = nvar

    def copy_in(n, k):
        def move(i, carry):
            where = pl.ds(pl.multiple_of(i * 8 * SUB, 8 * SUB), 8 * SUB)
            P[n, where, :] = conserved[k, where, :]
            return carry

        lax.fori_loop(0, rows * ring // (8 * SUB), move, 0, unroll=2)

    copy_in(slot, fields - 1)
    for t in range(tiles):
        edge = jnp.where(odd, RF[t], R[0, nvar - 1, 1, t])
        edge = jnp.where(local, edge, A[slots["mean_face"]])
        following = fix_polar(low, high, last, RF[t], edge, t)
        P[slot, layer(0, cells - 1, t), :] = 0.5 * (faces[nface - 1, layer(0, cells - 1, t), :] + following)
    copies.append(out(fields - 1, P.at[slot]))
    copies[-1].start()
    def hydro(k, carry):
        copy_in(k, k)
        for t in range(tiles):
            edge_l = jnp.where(local, sent_edge(R, 1, k, t), A[slots["mean_left"] + k])
            edge_r = jnp.where(local, sent_edge(R, 0, k, t), A[slots["mean_right"] + k])
            terms = halo_terms(
                A[slots["scale"] + k * tiles + t],
                [fix_polar(low, high, last, R[1, k, i, t], edge_l, t) for i in range(2)],
                [fix_polar(low, high, last, R[0, k, i, t], edge_r, t) for i in range(2)],
                [H[k, layer(2, cell, t), :] for cell in ends])
            for cell, term in zip(ends, terms):
                P[k, layer(0, cell, t), :] = P[k, layer(0, cell, t), :] + term
        out(k, P.at[k]).start()
        return carry

    lax.fori_loop(0, nvar, hydro, 0)
    copies += [out(k, P.at[k]) for k in range(nvar)]
    for c in copies:
        c.wait()


def blocked(x):
    n, rows, cells, theta = x.shape
    x = x.reshape(n, rows, cells // SUB, SUB, theta // LANES, LANES)
    return x.transpose(0, 1, 2, 4, 3, 5).reshape(n, rows * cells * (theta // LANES), LANES)


def unblocked(x, rows, cells, theta):
    x = x.reshape(x.shape[0], rows, cells // SUB, theta // LANES, SUB, LANES)
    return x.transpose(0, 1, 2, 4, 3, 5).reshape(x.shape[0], rows, cells, theta)


def body(nrow, nphi, hydro_vars, face_b, widths, diffusion):
    nvar, rows, cells, theta = hydro_vars.shape
    nface = face_b.shape[0]
    fields = nvar + nface
    cycles = widths.shape[0] // 2
    tiles = theta // LANES
    ring = cells * tiles
    f32 = jnp.float32
    shape = lambda *s: pltpu.VMEM(s, f32)
    far = pl.BlockSpec(memory_space=pltpu.HBM)
    near = pl.BlockSpec(memory_space=pltpu.VMEM)
    slots = late_slots(nvar, tiles)[1]
    held = ((fields + nface) * rows + nvar * (rows + 4)) * ring + (slots + (4 * nvar + 1) * tiles) * rows
    result_bytes = held * LANES * 4
    conserved, faces, *late = pl.pallas_call(
        functools.partial(kernel, nrow, nphi, rows, cells, tiles, cycles),
        out_shape=(
            pltpu.VMEM((fields, rows * ring, LANES), f32),
            pltpu.VMEM((nface, rows * ring, LANES), f32),
            pltpu.VMEM((slots, rows, LANES), f32),
            shape(nvar, (rows + 4) * ring, LANES),
            shape(2, nvar, 2, tiles, rows, LANES),
            shape(tiles, rows, LANES),
        ),
        in_specs=[far, far, far, far],
        out_specs=(near,) * 6,
        scratch_shapes=[
            shape(2, nvar, 2, tiles, rows, LANES),
            shape(tiles, rows, LANES),
            shape(ring, LANES),
            shape(rows * cells, LANES),
            shape(rows, LANES),
            shape(rows, LANES),
            shape(rows, LANES),
            shape(nphi // 2, rows, LANES),
            shape(2, rows, LANES),
            pltpu.SMEM((2 * cycles,), jnp.int32),
            shape(nvar, theta),
            pltpu.SemaphoreType.DMA((2,)),
            pltpu.SemaphoreType.DMA((fields,)),
            pltpu.SemaphoreType.DMA((2, nvar)),
            pltpu.SemaphoreType.DMA((2, nvar)),
            pltpu.SemaphoreType.DMA,
            pltpu.SemaphoreType.DMA,
            pltpu.SemaphoreType.DMA((nphi // 2,)),
            pltpu.SemaphoreType.DMA((nphi // 2,)),
            pltpu.SemaphoreType.DMA((3,)),
            pltpu.SemaphoreType.DMA((3,)),
            pltpu.SemaphoreType.REGULAR((nphi // 2,)),
            pltpu.SemaphoreType.REGULAR,
            pltpu.SemaphoreType.REGULAR,
        ],
        compiler_params=pltpu.CompilerParams(
            collective_id=0, has_side_effects=True, vmem_limit_bytes=LIMIT - result_bytes
        ),
        name="step",
    )(widths, blocked(hydro_vars), blocked(face_b), diffusion)
    conserved, faces = pl.pallas_call(
        functools.partial(spill, nvar, rows, cells, tiles, cycles),
        out_shape=(
            jax.ShapeDtypeStruct((fields, rows * ring, LANES), f32),
            jax.ShapeDtypeStruct((nface, rows * ring, LANES), f32),
        ),
        in_specs=[near] * 6,
        out_specs=(far, far),
        scratch_shapes=[shape(nvar + 1, rows * ring, LANES), pltpu.SemaphoreType.DMA((fields + nface,))],
        compiler_params=pltpu.CompilerParams(vmem_limit_bytes=4 * (nvar + 1) * rows * ring * LANES + 2000000),
        name="spill",
    )(conserved, faces, *late)
    return unblocked(conserved, rows, cells, theta), unblocked(faces, rows, cells, theta)


def solution(mesh):
    spec = P(None, "row", "phi", None)
    return jax.shard_map(
        functools.partial(body, mesh.shape["row"], mesh.shape["phi"]),
        mesh=mesh,
        in_specs=(spec, spec, P(), P()),
        out_specs=(spec, spec),
        check_vma=False,
    )
```
